32 devices in a mesh: gx: 4 (over x, core), gy: 4 (over z), gz: 2 (over y).
Axes of the slice: x: 2, y: 2, z: 4, core: 2. Of those that a mesh axis runs over, the one named last changes fastest.
Arguments:
- orbitals: float32 [16, 32, 32, 512], P(None, 'gx', 'gy', 'gz'), may hold values from -10 to 10
- potential: float32 [32, 32, 512], P('gx', 'gy', 'gz'), may hold values from 0 to 12
Outputs:
- updated: float32 [16, 32, 32, 512], P(None, 'gx', 'gy', 'gz')
- trial_energies: float32 [16], replicated
The draws below stay inside these ranges and needn't reach their ends.
All inputs are finite; a program needn't handle non-finite values.
Results may differ from the reference program's by a relative error of at most 0.000022.
Values sent between devices are 32-bit elements; how exact they have to be, the bound alone decides.
A program may use at most 64 MiB of HBM per device.

```python
import jax
import jax.numpy as jnp
from jax import lax

BANDS = 16
COARSE_SWEEPS = 4
NX = 32
NY = 32
NZ = 512


def draw_orbitals(key, part):
    position = jnp.arange(NX, dtype=jnp.float32) / NX
    noise = jnp.clip(jax.random.normal(jax.random.fold_in(key, 11), (BANDS, NX, NY, NZ), jnp.float32), -4.0, 4.0)
    envelope = jnp.exp(jnp.log(2.5) * position)
    return (noise * envelope[None, :, None, None]).astype(jnp.float32)


def draw_potential(key, part):
    position = jnp.arange(NX, dtype=jnp.float32) / NX
    rough = jax.random.uniform(jax.random.fold_in(key, 23), (NX, NY, NZ), jnp.float32, 0.0, 3.0)
    ramp = 6.0 * position
    return (rough + ramp[:, None, None]).astype(jnp.float32)


def setup_inputs(seed: int = 0) -> dict:
    key_list = jax.random.split(jax.random.key(seed), 3)
    orbitals = draw_orbitals(jax.random.fold_in(key_list[2], 71), 0)
    potential = draw_potential(jax.random.fold_in(key_list[2], 71), 0)
    return dict(orbitals=orbitals, potential=potential)


CENTRE_COEF = -2.5
NEAR_COEF = 4.0 / 3.0
FAR_COEF = -1.0 / 12.0
WEIGHT = 0.8
FINE_DIAG = 4.0
COARSE_DIAG = 1.75
EPSILON = 1e-6


def hamiltonian(values, potential):
    summed = (3.0 * CENTRE_COEF) * values
    for dimension in (0, 1, 2):
        summed = summed + NEAR_COEF * (jnp.roll(values, 1, dimension) + jnp.roll(values, -1, dimension))
        summed = summed + FAR_COEF * (jnp.roll(values, 2, dimension) + jnp.roll(values, -2, dimension))
    return -0.5 * summed + potential * values


def neighbours(values):
    beside_all = jnp.zeros_like(values)
    for dimension in (0, 1, 2):
        beside_all = beside_all + jnp.roll(values, 1, dimension) + jnp.roll(values, -1, dimension)
    return beside_all


def precondition(residual):
    smoothed = WEIGHT * residual / FINE_DIAG
    remainder = residual - (FINE_DIAG * smoothed - 0.5 * neighbours(smoothed))
    size_x, size_y, size_z = remainder.shape
    coarse_res = remainder.reshape(size_x // 2, 2, size_y // 2, 2, size_z // 2, 2).mean(axis=(1, 3, 5))
    approx = WEIGHT * coarse_res / COARSE_DIAG
    for sweep_index in range(COARSE_SWEEPS - 1):
        approx = approx + WEIGHT * (coarse_res - (COARSE_DIAG * approx - 0.125 * neighbours(approx))) / COARSE_DIAG
    lifted = jnp.repeat(jnp.repeat(jnp.repeat(approx, 2, 0), 2, 1), 2, 2)
    second = smoothed + lifted
    return second + WEIGHT * (residual - (FINE_DIAG * second - 0.5 * neighbours(second))) / FINE_DIAG


def one_band(wave, potential):
    applied = hamiltonian(wave, potential)
    energy = jnp.sum(wave * applied) / (jnp.sum(wave * wave) + EPSILON)
    residual = applied - energy * wave
    corrected = precondition(residual)
    applied_corr = hamiltonian(corrected, potential)
    response = applied_corr - energy * corrected
    lambda_step = -jnp.sum(residual * response) / (jnp.sum(response * response) + EPSILON)
    trial_wave = wave + lambda_step * corrected
    trial_applied = applied + lambda_step * applied_corr
    trial_energy = jnp.sum(trial_wave * trial_applied) / (jnp.sum(trial_wave * trial_wave) + EPSILON)
    residual_change = (trial_applied - trial_energy * trial_wave) - residual
    mixing_coef = -jnp.sum(residual * residual_change) / (jnp.sum(residual_change * residual_change) + EPSILON)
    mixed_res = residual + mixing_coef * residual_change
    updated = wave + (mixing_coef * lambda_step) * corrected + lambda_step * precondition(mixed_res)
    return updated, trial_energy


def reference(orbitals, potential):
    updated, trial_energies = lax.map(lambda wave: one_band(wave, potential), orbitals)
    return updated, trial_energies
```

```python
import functools

import jax
import jax.numpy as jnp
from jax import lax
from jax.experimental import pallas as pl
from jax.experimental.pallas import tpu as pltpu
from jax.sharding import PartitionSpec as P

COARSE_SWEEPS = 4
WEIGHT = 0.8
COARSE_DIAG = 1.75
EPSILON = 1e-06
LANES = 128
ROWS = 8
GROUPS = 2
AXES = ("gx", "gy", "gz")
MESH = pl.DeviceIdType.MESH
NDOTS = 8

PACK, APPLY, PREPARE, SWEEP = 0.35, 1.2, 1.1, 0.5
FINE_LINK, COARSE_LINK = 1.4, 0.35
HALO, PLANE, MIDDLE, START = 3.5, 2.0, 0.1, 2.0


def kernel(sizes, orb_hbm, pot, out, energies, *scratch):
    (
        orb, app, res, cor, rsp, rem, coarse,
        fys, fyr, fzs, fzr, hy, cxs, cxr, cys, cyr, czs, czr, hcy,
        acc, scal, red, load_sem, send_sem, recv_sem, rsend, rrecv,
    ) = scratch
    nx, ny, nz = sizes
    bands, xs = orb_hbm.shape[0], orb_hbm.shape[1]
    tiles = orb_hbm.shape[3] // LANES
    xc = xs // 2
    per = bands // GROUPS
    zper = min(per, 8)
    me = [lax.axis_index(a) for a in AXES]
    right = [lax.rem(m + 1, n) for m, n in zip(me, sizes)]
    left = [lax.rem(m + n - 1, n) for m, n in zip(me, sizes)]

    loads = [
        [
            pltpu.make_async_copy(
                orb_hbm.at[pl.ds(g * per, per), :, :, pl.ds(t * LANES, LANES)],
                orb.at[pl.ds(g * per, per), pl.ds(2, xs), t],
                load_sem.at[g, t],
            )
            for t in range(tiles)
        ]
        for g in range(GROUPS)
    ]
    for group in loads:
        for c in group:
            c.start()

    plane = [
        {"gx": lax.rem(me[0] + d // nz, nx), "gz": lax.rem(me[2] + d % nz, nz)} for d in range(1, nx * nz)
    ]
    column = [{"gy": lax.rem(me[1] + d, ny)} for d in range(1, ny)]
    barrier = pltpu.get_barrier_semaphore()
    for to in plane + column:
        pl.semaphore_signal(barrier, inc=1, device_id=to, device_id_type=MESH)
    energies[...] = jnp.zeros_like(energies)

    row = lax.broadcasted_iota(jnp.int32, (ROWS, LANES), 0)
    lane = lax.broadcasted_iota(jnp.int32, (ROWS, LANES), 1)
    even_lane = lane % 2 == 0
    even_row = row % 2 == 0
    low_half = lane < LANES // 2
    first_of_four = lane % 4 < 2

    def roll(v, k, axis):
        return pltpu.roll(v, k % v.shape[axis], axis)

    def flat(ref):
        n = 1
        for s in ref.shape[:-1]:
            n *= s
        return ref.reshape(n, LANES)

    def loop(lo, hi, f):
        def step(i, carry):
            f(i)
            return carry

        lax.fori_loop(lo, hi, step, 0)

    def remote(src, dst, slot, k, axis, target):
        return pltpu.make_async_remote_copy(
            src_ref=src,
            dst_ref=dst,
            send_sem=send_sem.at[slot, k],
            recv_sem=recv_sem.at[slot, k],
            device_id={axis: target},
            device_id_type=MESH,
        )

    def z_copies(src, dst_l, dst_r, slot):
        copies = [remote(src, dst_l, slot, 4, "gz", right[2])]
        if nz > 2:
            copies.append(remote(src, dst_r, slot, 5, "gz", left[2]))
        return copies

    def fine_send(field, which, depth, g):
        lo = g * per
        view = flat(field)
        span = field.shape[1]
        ys, yr = fys[which], fyr[which]
        zs, zr = fzs[which], fzr[which]

        def pack(b):
            for t in range(tiles):
                for j in range(depth):
                    base = ((b * span + 2) * tiles + t) * ROWS
                    ys[0, b, j, t] = view[pl.ds(base + ROWS - depth + j, xs, stride=tiles * ROWS), :]
                    ys[1, b, j, t] = view[pl.ds(base + j, xs, stride=tiles * ROWS), :]
            packed = jnp.zeros((ROWS, LANES), jnp.float32)
            for x in range(xs):
                w = jnp.where(low_half, field[b, 2 + x, 0], field[b, 2 + x, tiles - 1])
                packed = jnp.where(lane // 4 == x, roll(w, 2 + 4 * x, 1), packed)
            zs[b] = packed

        loop(lo, lo + per, pack)
        slot = which * GROUPS + g
        part = pl.ds(lo, per)
        copies = [
            remote(field.at[part, pl.ds(2 + xs - depth, depth)], field.at[part, pl.ds(2 - depth, depth)], slot, 0, "gx", right[0]),
            remote(field.at[part, pl.ds(2, depth)], field.at[part, pl.ds(2 + xs, depth)], slot, 1, "gx", left[0]),
            remote(ys.at[0, part], yr.at[0, part], slot, 2, "gy", right[1]),
            remote(ys.at[1, part], yr.at[1, part], slot, 3, "gy", left[1]),
        ] + z_copies(zs.at[part], zr.at[0, part], zr.at[1, part], slot)
        for c in copies:
            c.start()
        return copies

    def wait(copies):
        for c in copies:
            c.wait()

    def z_packed(zr, b):
        if nz > 2:
            return jnp.where(first_of_four, zr[0, b], zr[1, b])
        return zr[0, b]

    def unpack_y(yr, b, depth):
        view = flat(hy)
        for t in range(tiles):
            for j in range(depth):
                base = (b * xs * tiles + t) * ROWS
                view[pl.ds(base + ROWS - depth + j, xs, stride=tiles * ROWS), :] = yr(0, j, t)
                view[pl.ds(base + j, xs, stride=tiles * ROWS), :] = yr(1, j, t)

    def shifted_y(v, h, k):
        up = roll(jnp.where(row >= ROWS - k, h, v), k, 0)
        down = roll(jnp.where(row < k, h, v), -k, 0)
        return up + down

    def shifted_z(vs, hz, k):
        before = [hz] + vs[:-1]
        after = vs[1:] + [hz]
        return [
            roll(jnp.where(lane >= LANES - k, p, v), k, 1) + roll(jnp.where(lane < k, n, v), -k, 1)
            for p, v, n in zip(before, vs, after)
        ]

    def hamiltonian(field, which, b, use):
        unpack_y(lambda s, j, t: fyr[which][s, b, j, t], b, 2)
        zp = z_packed(fzr[which], b)
        for x in range(xs):
            hz = roll(zp, -(4 * x + 2), 1)
            vs = [field[b, 2 + x, t] for t in range(tiles)]
            z1, z2 = shifted_z(vs, hz, 1), shifted_z(vs, hz, 2)
            outs = []
            for t in range(tiles):
                h = hy[b, x, t]
                near = field[b, 1 + x, t] + field[b, 3 + x, t] + shifted_y(vs[t], h, 1) + z1[t]
                far = field[b, x, t] + field[b, 4 + x, t] + shifted_y(vs[t], h, 2) + z2[t]
                potential = pot[x, :, t * LANES : (t + 1) * LANES]
                outs.append((potential + 3.75) * vs[t] - (2.0 / 3.0) * near + (1.0 / 24.0) * far)
            use(x, vs, outs)

    def rowsum(vs):
        return jnp.sum(functools.reduce(jnp.add, vs), axis=0, keepdims=True)

    def reduce_send(k, stage, peers, here, value):
        slot = here + stage * nx * nz
        red[k, slot] = value
        copies = [
            pltpu.make_async_remote_copy(
                src_ref=red.at[k, slot],
                dst_ref=red.at[k, slot],
                send_sem=rsend.at[k, stage * nx * nz + d],
                recv_sem=rrecv.at[k, stage * nx * nz + d],
                device_id=to,
                device_id_type=MESH,
            )
            for d, to in enumerate(peers)
        ]
        for c in copies:
            c.start()
        return copies

    def reduce_start(index, g, ndots):
        total = jnp.zeros((ROWS, LANES), jnp.float32)
        for i in range(ndots * per // ROWS):
            part = jnp.sum(acc[index, g, i * ROWS : (i + 1) * ROWS, :], axis=1, keepdims=True)
            total = jnp.where(lane == row + i * ROWS, part, total)
        k = index * GROUPS + g
        return reduce_send(k, 0, plane, me[0] * nz + me[2], jnp.sum(total, axis=0, keepdims=True))

    def reduce_rows(k, first, count):
        total = red[k, first]
        for i in range(1, count):
            total = total + red[k, first + i]
        return total

    def reduce_middle(index, g, copies):
        k = index * GROUPS + g
        wait(copies)
        return reduce_send(k, 1, column, me[1], reduce_rows(k, 0, nx * nz))

    def reduce_finish(index, g, ndots, copies):
        k = index * GROUPS + g
        wait(copies)
        total = jnp.broadcast_to(reduce_rows(k, nx * nz, ny), (ROWS, LANES))
        return [total if q == 0 else roll(total, -q * per, 1) for q in range(ndots)]

    def put(k, g, values):
        for b in range(per):
            scal[k, g * per + b : g * per + b + 1, :] = jnp.broadcast_to(values[0:1, b : b + 1], (1, LANES))

    def get(k, b):
        return scal[k, pl.ds(b, 1), :]

    def restrict(b, ry, rz):
        unpack_y(ry, b, 1)
        for X in range(xc):
            pair = [None] * tiles
            for x in (2 * X, 2 * X + 1):
                hz = roll(rz, -(4 * x + 2), 1)
                vs = [res[b, 2 + x, t] for t in range(tiles)]
                z1 = shifted_z(vs, hz, 1)
                for t in range(tiles):
                    s = res[b, 1 + x, t] + res[b, 3 + x, t] + shifted_y(vs[t], hy[b, x, t], 1) + z1[t]
                    m = (1.0 - WEIGHT) * vs[t] + (0.5 * WEIGHT / 4.0) * s
                    rem[b, x, t] = m
                    pair[t] = m if pair[t] is None else pair[t] + m
            for t in range(tiles):
                s = pair[t]
                s = s + jnp.where(even_row, roll(s, -1, 0), roll(s, 1, 0))
                s = s + jnp.where(even_lane, roll(s, -1, 1), roll(s, 1, 1))
                coarse[0, b, 1 + X, t] = s * (0.125 * WEIGHT / COARSE_DIAG)

    def coarse_send(which, level, g):
        cf = coarse.at[level]
        view = flat(coarse)
        lo = g * per // 4

        def pack(i):
            b = 4 * i
            for t in range(tiles):
                for side, X in ((0, xc), (1, 1)):
                    lanes = [
                        jnp.where(even_lane, cf[b + k, X, t], cf[b + k + 1, X, t]) for k in (0, 2)
                    ]
                    cxs[which, side, i, t] = jnp.where(even_row, lanes[0], lanes[1])
                for side, j in ((0, ROWS - 1), (1, 0)):
                    vs = [
                        view[pl.ds((((level * bands + b + k) * (xc + 2) + 1) * tiles + t) * ROWS + j, xc, stride=tiles * ROWS), :]
                        for k in range(4)
                    ]
                    ev = even_lane[:xc]
                    cys[which, side, i, t, 0:xc] = jnp.where(ev, vs[0], vs[1])
                    cys[which, side, i, t, xc : 2 * xc] = jnp.where(ev, vs[2], vs[3])

        loop(lo, lo + per // 4, pack)

        def pack_z(i):
            packed = jnp.zeros((ROWS, LANES), jnp.float32)
            for k in range(zper):
                for X in range(xc):
                    off = 4 * (k * xc + X)
                    w = jnp.where(low_half, cf[zper * i + k, 1 + X, 0], cf[zper * i + k, 1 + X, tiles - 1])
                    packed = jnp.where(lane // 4 == off // 4, roll(w, 2 + off, 1), packed)
            czs[which, i] = packed

        loop(g * per // zper, (g + 1) * per // zper, pack_z)
        slot = (4 + which) * GROUPS + g
        part = pl.ds(lo, per // 4)
        zpart = pl.ds(g * per // zper, per // zper)
        copies = [
            remote(cxs.at[which, 0, part], cxr.at[which, 0, part], slot, 0, "gx", right[0]),
            remote(cxs.at[which, 1, part], cxr.at[which, 1, part], slot, 1, "gx", left[0]),
            remote(cys.at[which, 0, part], cyr.at[which, 0, part], slot, 2, "gy", right[1]),
            remote(cys.at[which, 1, part], cyr.at[which, 1, part], slot, 3, "gy", left[1]),
        ] + z_copies(czs.at[which, zpart], czr.at[which, 0, zpart], czr.at[which, 1, zpart], slot)
        for c in copies:
            c.start()
        return copies

    def spread_lanes(p):
        return (
            jnp.where(even_lane, p, roll(p, 1, 1)),
            jnp.where(even_lane, roll(p, -1, 1), p),
        )

    def coarse_unpack(which, level, g):
        cf = coarse.at[level]
        view = flat(hcy)
        lo = g * per // 4

        def unpack(i):
            b = 4 * i
            for t in range(tiles):
                for side, X in ((0, 0), (1, xc + 1)):
                    p = cxr[which, side, i, t]
                    top = jnp.where(even_row, p, roll(p, 1, 0))
                    low = jnp.where(even_row, roll(p, -1, 0), p)
                    for k, v in enumerate(spread_lanes(top) + spread_lanes(low)):
                        cf[b + k, X, t] = v
                for side, j in ((0, ROWS - 2), (1, 0)):
                    first, second = spread_lanes(cyr[which, side, i, t])
                    for k, v in enumerate((first[:xc], second[:xc], first[xc:], second[xc:])):
                        base = ((b + k) * xc * tiles + t) * ROWS + j
                        for dup in range(2):
                            view[pl.ds(base + dup, xc, stride=tiles * ROWS), :] = v

        loop(lo, lo + per // 4, unpack)

    def coarse_loop(which, g, f):
        def bundle(i):
            zp = czr[which, 0, i]
            if nz > 2:
                zp = jnp.where(first_of_four, zp, czr[which, 1, i])
            for k in range(zper):
                f(zper * i + k, lambda X, k=k: roll(zp, -(4 * (k * xc + X) + 2), 1))

        loop(g * per // zper, (g + 1) * per // zper, bundle)

    def sweep(which, level, g):
        coarse_unpack(which, level, g)

        def one(b, hz):
            for X in range(xc):
                vs = [coarse[level, b, 1 + X, t] for t in range(tiles)]
                z = shifted_z(vs, hz(X), 2)
                for t in range(tiles):
                    s = coarse[level, b, X, t] + coarse[level, b, 2 + X, t] + shifted_y(vs[t], hcy[b, X, t], 2) + z[t]
                    rhs = coarse[0, b, 1 + X, t]
                    coarse[level + 1, b, 1 + X, t] = (
                        (1.0 - WEIGHT) * vs[t] + (0.125 * WEIGHT / COARSE_DIAG) * s + rhs
                    )

        coarse_loop(which, g, one)

    def prolong(which, level, g, use):
        coarse_unpack(which, level, g)

        def one(b, hz):
            for X in range(xc):
                vs = [coarse[level, b, 1 + X, t] for t in range(tiles)]
                z = shifted_z(vs, hz(X), 1)
                for t in range(tiles):
                    s = shifted_y(vs[t], hcy[b, X, t], 1) + z[t] + vs[t]
                    for x, other in ((2 * X, X), (2 * X + 1, 2 + X)):
                        total = s + coarse[level, b, other, t]
                        kr = (1.0 - WEIGHT) * (res[b, 2 + x, t] + vs[t] + rem[b, x, t]) + (
                            0.5 * WEIGHT / 4.0
                        ) * total
                        use(b, x, t, kr)

        coarse_loop(which, g, one)

    def apply_one(g, b):
        norm, energy = [], []

        def use(x, vs, outs):
            for t in range(tiles):
                app[b, 2 + x, t] = outs[t]
                norm.append(vs[t] * vs[t])
                energy.append(vs[t] * outs[t])

        hamiltonian(orb, 0, b, use)
        acc[0, g, pl.ds(b - g * per, 1), :] = rowsum(norm)
        acc[0, g, pl.ds(b - g * per + per, 1), :] = rowsum(energy)

    def prepare_first(b):
        e = get(0, b)
        for x in range(1, xs + 3):
            for t in range(tiles):
                res[b, x, t] = app[b, x, t] - e * orb[b, x, t]

        def ry(s, j, t):
            return fyr[1][s, b, 0, t] - e * fyr[0][s, b, 1 - s, t]

        restrict(b, ry, z_packed(fzr[1], b) - e * z_packed(fzr[0], b))

    def use_first(b, x, t, kr):
        cor[b, 2 + x, t] = kr

    def respond_one(g, b):
        e = get(0, b)
        dots = [None] * NDOTS

        def use(x, vs, outs):
            for t in range(tiles):
                c, o, r = vs[t], orb[b, 2 + x, t], res[b, 2 + x, t]
                p = outs[t] - e * c
                rsp[b, 2 + x, t] = p
                for q, (u, v) in enumerate(((r, p), (p, p), (o, c), (c, c), (p, o), (p, c), (r, o), (r, c))):
                    w = u * v
                    dots[q] = w if dots[q] is None else dots[q] + w

        hamiltonian(cor, 2, b, use)
        for q in range(NDOTS):
            acc[1, g, pl.ds(b - g * per + q * per, 1), :] = rowsum([dots[q]])

    def prepare_second(b):
        e, ml, mc, mcl = get(0, b), get(2, b), get(3, b), get(4, b)

        def mixed(r, p, o, c):
            return r + ml * p - mc * o - mcl * c

        for x in range(1, xs + 3):
            for t in range(tiles):
                res[b, x, t] = mixed(res[b, x, t], rsp[b, x, t], orb[b, x, t], cor[b, x, t])

        def ry(s, j, t):
            o = fyr[0][s, b, 1 - s, t]
            r = fyr[1][s, b, 0, t] - e * o
            return mixed(r, fyr[3][s, b, 0, t], o, fyr[2][s, b, 1 - s, t])

        oz = z_packed(fzr[0], b)
        rz = z_packed(fzr[1], b) - e * oz
        restrict(b, ry, mixed(rz, z_packed(fzr[3], b), oz, z_packed(fzr[2], b)))

    def use_second(b, x, t, kr):
        out[b, x, :, t * LANES : (t + 1) * LANES] = (
            orb[b, 2 + x, t] + get(2, b) * cor[b, 2 + x, t] + get(1, b) * kr
        )

    def precondition(base, g, prepare, use):
        loop(g * per, (g + 1) * per, prepare)
        flight = coarse_send(base, 0, g)
        yield PREPARE, COARSE_LINK, HALO
        for s in range(COARSE_SWEEPS - 1):
            wait(flight)
            sweep(base + s, s, g)
            flight = coarse_send(base + s + 1, s + 1, g)
            yield SWEEP, COARSE_LINK, HALO
        wait(flight)
        prolong(base + COARSE_SWEEPS - 1, COARSE_SWEEPS - 1, g, use)

    def chain(g):
        lo, hi = g * per, (g + 1) * per
        wait(loads[g])
        flight = fine_send(orb, 0, 2, g)
        yield PACK, 2 * FINE_LINK, HALO
        wait(flight)
        loop(lo, hi, functools.partial(apply_one, g))
        sums = reduce_start(0, g, 2)
        flight = fine_send(app, 1, 1, g)
        yield APPLY, FINE_LINK, PLANE
        sums = reduce_middle(0, g, sums)
        yield MIDDLE, 0.0, HALO
        norm_orbitals, first_energy = reduce_finish(0, g, 2, sums)
        energy = first_energy / (norm_orbitals + EPSILON)
        put(0, g, energy)
        wait(flight)
        yield from precondition(0, g, prepare_first, use_first)
        flight = fine_send(cor, 2, 2, g)
        yield SWEEP + PACK, 2 * FINE_LINK, HALO
        wait(flight)
        loop(lo, hi, functools.partial(respond_one, g))
        sums = reduce_start(1, g, NDOTS)
        flight = fine_send(rsp, 3, 1, g)
        yield APPLY, FINE_LINK, PLANE
        sums = reduce_middle(1, g, sums)
        yield MIDDLE, 0.0, HALO
        rp, pp, oc, cc, po, pc, ro, rc = reduce_finish(1, g, NDOTS, sums)
        lam = -rp / (pp + EPSILON)
        trial_norm = norm_orbitals + 2.0 * lam * oc + lam * lam * cc
        trial_sum = (
            first_energy + lam * ((po + energy * oc) + (rc + energy * oc)) + lam * lam * (pc + energy * cc)
        )
        trial = trial_sum / (trial_norm + EPSILON)
        mine = jnp.where(lane < per, trial, 0.0)
        energies[...] = energies[...] + (mine if g == 0 else roll(mine, g * per, 1))
        change = trial - energy
        projected = lam * rp - change * (ro + lam * rc)
        cross = po + lam * pc
        change_norm = lam * lam * pp - 2.0 * lam * change * cross + change * change * trial_norm
        mix = -projected / (change_norm + EPSILON)
        put(1, g, lam)
        put(2, g, mix * lam)
        put(3, g, mix * change)
        put(4, g, mix * change * lam)
        wait(flight)
        yield from precondition(COARSE_SWEEPS, g, prepare_second, use_second)
        yield SWEEP, 0.0, 0.0

    pl.semaphore_wait(barrier, len(plane) + len(column))
    chains = [chain(g) for g in range(GROUPS)]
    ready = [START * g for g in range(GROUPS)]
    now = link = 0.0
    while any(c is not None for c in chains):
        g = min((g for g in range(GROUPS) if chains[g] is not None), key=lambda g: (ready[g], g))
        step = next(chains[g], None)
        if step is None:
            chains[g] = None
            continue
        work, load, latency = step
        now = max(now, ready[g]) + work
        link = max(link, now) + load
        ready[g] = link + latency


def solution(mesh):
    sizes = tuple(mesh.shape[a] for a in AXES)

    def body(orbitals, potential):
        bands, xs, ys, zs = orbitals.shape
        tiles = zs // LANES
        tile = (ROWS, LANES)
        vmem = lambda *s: pltpu.VMEM(s + tile, jnp.float32)
        field = vmem(bands, xs + 4, tiles)
        exchanges = 4 + 2 * COARSE_SWEEPS
        faces = (2 * COARSE_SWEEPS, 2, bands // 4, tiles)
        slots = sizes[0] * sizes[2] + sizes[1]
        per = bands // GROUPS
        zbundles = bands // min(per, 8)

        def call(*refs):
            refs = list(refs)
            head, rest = refs[:4], refs[4:]
            fields, rest = rest[:7], rest[7:]
            fys, rest = rest[:4], rest[4:]
            fyr, rest = rest[:4], rest[4:]
            fzs, rest = rest[:4], rest[4:]
            fzr, rest = rest[:4], rest[4:]
            kernel(sizes, *head, *fields, fys, fyr, fzs, fzr, *rest)

        depths = (2, 1, 2, 1)
        updated, trial = pl.pallas_call(
            call,
            out_shape=(
                jax.ShapeDtypeStruct(orbitals.shape, jnp.float32),
                jax.ShapeDtypeStruct(tile, jnp.float32),
            ),
            in_specs=[
                pl.BlockSpec(memory_space=pl.ANY),
                pl.BlockSpec(memory_space=pltpu.VMEM),
            ],
            out_specs=(
                pl.BlockSpec(memory_space=pltpu.VMEM),
                pl.BlockSpec(memory_space=pltpu.VMEM),
            ),
            scratch_shapes=[field] * 5
            + [vmem(bands, xs, tiles), vmem(COARSE_SWEEPS, bands, xs // 2 + 2, tiles)]
            + [vmem(2, bands, d, tiles) for d in depths]
            + [vmem(2, bands, d, tiles) for d in depths]
            + [vmem(bands) for d in depths]
            + [vmem(2, bands) for d in depths]
            + [
                vmem(bands, xs, tiles),
                vmem(*faces),
                vmem(*faces),
                vmem(*faces),
                vmem(*faces),
                vmem(2 * COARSE_SWEEPS, zbundles),
                vmem(2 * COARSE_SWEEPS, 2, zbundles),
                vmem(bands, xs // 2, tiles),
                pltpu.VMEM((2, GROUPS, NDOTS * per, LANES), jnp.float32),
                pltpu.VMEM((5, bands, LANES), jnp.float32),
                pltpu.VMEM((2 * GROUPS, slots, 1, LANES), jnp.float32),
                pltpu.SemaphoreType.DMA((GROUPS, tiles)),
                pltpu.SemaphoreType.DMA((exchanges * GROUPS, 6)),
                pltpu.SemaphoreType.DMA((exchanges * GROUPS, 6)),
                pltpu.SemaphoreType.DMA((2 * GROUPS, slots)),
                pltpu.SemaphoreType.DMA((2 * GROUPS, slots)),
            ],
            compiler_params=pltpu.CompilerParams(
                collective_id=0, has_side_effects=True, vmem_limit_bytes=48 * 1024 * 1024
            ),
        )(orbitals, potential)
        return updated, trial[0, :bands]

    return jax.shard_map(
        body,
        mesh=mesh,
        in_specs=(P(None, "gx", "gy", "gz"), P("gx", "gy", "gz")),
        out_specs=(P(None, "gx", "gy", "gz"), P()),
        check_vma=False,
    )
```

```python
import functools

import jax
import jax.numpy as jnp
from jax import lax
from jax.experimental import pallas as pl
from jax.experimental.pallas import tpu as pltpu
from jax.sharding import PartitionSpec as P

COARSE_SWEEPS = 4
WEIGHT = 0.8
COARSE_DIAG = 1.75
EPSILON = 1e-06
LANES = 128
ROWS = 8
GROUPS = 4
AXES = ("gx", "gy", "gz")
MESH = pl.DeviceIdType.MESH
NDOTS = 8


def kernel(sizes, orb_hbm, pot_hbm, out, energies, *scratch):
    (
        orb, app, res, cor, rsp, rem, coarse,
        fys, fyr, fzs, fzr, hy, cxs, cxr, cys, cyr, czs, czr, hcy,
        acc, scal, keep, red, pot, load_sem, send_sem, recv_sem, rsend, rrecv,
    ) = scratch
    nx, ny, nz = sizes
    bands, xs = orb_hbm.shape[0], orb_hbm.shape[1]
    tiles = orb_hbm.shape[3] // LANES
    xc = xs // 2
    per = bands // GROUPS
    zper = min(per, 8)
    devices = nx * ny * nz
    me = [lax.axis_index(a) for a in AXES]
    right = [lax.rem(m + 1, n) for m, n in zip(me, sizes)]
    left = [lax.rem(m + n - 1, n) for m, n in zip(me, sizes)]

    here = (me[0] * ny + me[1]) * nz + me[2]

    def start(copies):
        for c in copies:
            c.start()

    def wait(copies):
        for c in copies:
            c.wait()

    pot_load = pltpu.make_async_copy(pot_hbm, pot, load_sem.at[GROUPS, 0])

    def load_copies(g):
        part = pl.ds(g * per, per)
        return [
            pltpu.make_async_copy(
                orb_hbm.at[part, :, :, pl.ds(t * LANES, LANES)],
                orb.at[part, pl.ds(2, xs), t],
                load_sem.at[g, t],
            )
            for t in range(tiles)
        ]

    for g in range(GROUPS):
        start(load_copies(g))
    pot_load.start()

    def wrap(k, d):
        return lax.rem(me[k] + d, sizes[k])

    def every_peer(f):
        if devices <= 64:
            xyz = [[me[k]] + [wrap(k, d) for d in range(1, sizes[k])] for k in range(3)]
            for d in range(1, devices):
                f((xyz[0][d // (ny * nz)], xyz[1][d // nz % ny], xyz[2][d % nz]))
        else:

            def step(d, carry):
                f((wrap(0, d // (ny * nz)), wrap(1, lax.rem(d // nz, ny)), wrap(2, lax.rem(d, nz))))
                return carry

            lax.fori_loop(1, devices, step, 0)

    barrier = pltpu.get_barrier_semaphore()
    every_peer(lambda to: pl.semaphore_signal(barrier, inc=1, device_id=to, device_id_type=MESH))

    row = lax.broadcasted_iota(jnp.int32, (ROWS, LANES), 0)
    lane = lax.broadcasted_iota(jnp.int32, (ROWS, LANES), 1)
    even_lane = lane % 2 == 0
    even_row = row % 2 == 0
    low_half = lane < LANES // 2
    first_of_four = lane % 4 < 2

    def roll(v, k, axis):
        return pltpu.roll(v, k % v.shape[axis], axis)

    def flat(ref):
        n = 1
        for s in ref.shape[:-1]:
            n *= s
        return ref.reshape(n, LANES)

    def loop(lo, hi, f):
        def step(i, carry):
            f(i)
            return carry

        lax.fori_loop(lo, hi, step, 0)

    def remote(src, dst, slot, k, axis, target):
        return pltpu.make_async_remote_copy(
            src_ref=src,
            dst_ref=dst,
            send_sem=send_sem.at[slot, k],
            recv_sem=recv_sem.at[slot, k],
            device_id={axis: target},
            device_id_type=MESH,
        )

    def z_copies(src, dst_l, dst_r, slot):
        copies = [remote(src, dst_l, slot, 4, "gz", right[2])]
        if nz > 2:
            copies.append(remote(src, dst_r, slot, 5, "gz", left[2]))
        return copies

    def fine_copies(field, which, depth, g):
        slot = which * GROUPS + g
        part = pl.ds(g * per, per)
        ys, yr = fys[which], fyr[which]
        zs, zr = fzs[which], fzr[which]
        return [
            remote(field.at[part, pl.ds(2 + xs - depth, depth)], field.at[part, pl.ds(2 - depth, depth)], slot, 0, "gx", right[0]),
            remote(field.at[part, pl.ds(2, depth)], field.at[part, pl.ds(2 + xs, depth)], slot, 1, "gx", left[0]),
            remote(ys.at[0, part], yr.at[0, part], slot, 2, "gy", right[1]),
            remote(ys.at[1, part], yr.at[1, part], slot, 3, "gy", left[1]),
        ] + z_copies(zs.at[part], zr.at[0, part], zr.at[1, part], slot)

    def fine_send(field, which, depth, g):
        view = flat(field)
        span = field.shape[1]
        ys, zs = fys[which], fzs[which]

        def pack(b):
            for t in range(tiles):
                for j in range(depth):
                    base = ((b * span + 2) * tiles + t) * ROWS
                    ys[0, b, j, t] = view[pl.ds(base + ROWS - depth + j, xs, stride=tiles * ROWS), :]
                    ys[1, b, j, t] = view[pl.ds(base + j, xs, stride=tiles * ROWS), :]
            packed = jnp.zeros((ROWS, LANES), jnp.float32)
            for x in range(xs):
                w = jnp.where(low_half, field[b, 2 + x, 0], field[b, 2 + x, tiles - 1])
                packed = jnp.where(lane // 4 == x, roll(w, 2 + 4 * x, 1), packed)
            zs[b] = packed

        loop(g * per, (g + 1) * per, pack)
        start(fine_copies(field, which, depth, g))

    def z_packed(zr, b):
        if nz > 2:
            return jnp.where(first_of_four, zr[0, b], zr[1, b])
        return zr[0, b]

    def unpack_y(yr, b, depth):
        view = flat(hy)
        for t in range(tiles):
            for j in range(depth):
                base = (b * xs * tiles + t) * ROWS
                view[pl.ds(base + ROWS - depth + j, xs, stride=tiles * ROWS), :] = yr(0, j, t)
                view[pl.ds(base + j, xs, stride=tiles * ROWS), :] = yr(1, j, t)

    def shifted_y(v, h, k):
        up = roll(jnp.where(row >= ROWS - k, h, v), k, 0)
        down = roll(jnp.where(row < k, h, v), -k, 0)
        return up + down

    def shifted_z(vs, hz, k):
        before = [hz] + vs[:-1]
        after = vs[1:] + [hz]
        return [
            roll(jnp.where(lane >= LANES - k, p, v), k, 1) + roll(jnp.where(lane < k, n, v), -k, 1)
            for p, v, n in zip(before, vs, after)
        ]

    def hamiltonian(field, which, b, use):
        unpack_y(lambda s, j, t: fyr[which][s, b, j, t], b, 2)
        zp = z_packed(fzr[which], b)
        for x in range(xs):
            hz = roll(zp, -(4 * x + 2), 1)
            vs = [field[b, 2 + x, t] for t in range(tiles)]
            z1, z2 = shifted_z(vs, hz, 1), shifted_z(vs, hz, 2)
            outs = []
            for t in range(tiles):
                h = hy[b, x, t]
                near = field[b, 1 + x, t] + field[b, 3 + x, t] + shifted_y(vs[t], h, 1) + z1[t]
                far = field[b, x, t] + field[b, 4 + x, t] + shifted_y(vs[t], h, 2) + z2[t]
                potential = pot[x, :, t * LANES : (t + 1) * LANES]
                outs.append((potential + 3.75) * vs[t] - (2.0 / 3.0) * near + (1.0 / 24.0) * far)
            use(x, vs, outs)

    def rowsum(vs):
        return jnp.sum(functools.reduce(jnp.add, vs), axis=0, keepdims=True)

    def reduce_start(index, g, ndots):
        total = jnp.zeros((ROWS, LANES), jnp.float32)
        for i in range(ndots * per // ROWS):
            part = jnp.sum(acc[index, g, i * ROWS : (i + 1) * ROWS, :], axis=1, keepdims=True)
            total = jnp.where(lane == row + i * ROWS, part, total)
        k = index * GROUPS + g
        red[k, here] = jnp.sum(total, axis=0, keepdims=True)

        def send(to):
            pltpu.make_async_remote_copy(
                src_ref=red.at[k, here],
                dst_ref=red.at[k, here],
                send_sem=rsend.at[k],
                recv_sem=rrecv.at[k],
                device_id=to,
                device_id_type=MESH,
            ).start()

        every_peer(send)

    def reduce_finish(index, g, ndots):
        k = index * GROUPS + g
        rest = red.at[k, pl.ds(0, devices - 1)]
        pltpu.make_async_copy(rest, rest, rrecv.at[k]).wait()
        pltpu.make_async_copy(rest, rest, rsend.at[k]).wait()
        total = jnp.broadcast_to(jnp.sum(red[k], axis=0), (ROWS, LANES))
        return [total if q == 0 else roll(total, -q * per, 1) for q in range(ndots)]

    def put(k, g, values):
        for b in range(per):
            scal[k, pl.ds(g * per + b, 1), :] = jnp.broadcast_to(values[0:1, b : b + 1], (1, LANES))

    def get(k, b):
        return scal[k, pl.ds(b, 1), :]

    def restrict(b, ry, rz):
        unpack_y(ry, b, 1)
        for X in range(xc):
            pair = [None] * tiles
            for x in (2 * X, 2 * X + 1):
                hz = roll(rz, -(4 * x + 2), 1)
                vs = [res[b, 2 + x, t] for t in range(tiles)]
                z1 = shifted_z(vs, hz, 1)
                for t in range(tiles):
                    s = res[b, 1 + x, t] + res[b, 3 + x, t] + shifted_y(vs[t], hy[b, x, t], 1) + z1[t]
                    m = (1.0 - WEIGHT) * vs[t] + (0.5 * WEIGHT / 4.0) * s
                    rem[b, x, t] = m
                    pair[t] = m if pair[t] is None else pair[t] + m
            for t in range(tiles):
                s = pair[t]
                s = s + jnp.where(even_row, roll(s, -1, 0), roll(s, 1, 0))
                s = s + jnp.where(even_lane, roll(s, -1, 1), roll(s, 1, 1))
                coarse[0, b, 1 + X, t] = s * (0.125 * WEIGHT / COARSE_DIAG)

    def coarse_copies(which, g):
        slot = (4 + which) * GROUPS + g
        part = pl.ds(g * (per // 4), per // 4)
        zpart = pl.ds(g * (per // zper), per // zper)
        return [
            remote(cxs.at[which, 0, part], cxr.at[which, 0, part], slot, 0, "gx", right[0]),
            remote(cxs.at[which, 1, part], cxr.at[which, 1, part], slot, 1, "gx", left[0]),
            remote(cys.at[which, 0, part], cyr.at[which, 0, part], slot, 2, "gy", right[1]),
            remote(cys.at[which, 1, part], cyr.at[which, 1, part], slot, 3, "gy", left[1]),
        ] + z_copies(czs.at[which, zpart], czr.at[which, 0, zpart], czr.at[which, 1, zpart], slot)

    def coarse_send(which, level, g):
        cf = coarse.at[level]
        view = flat(coarse)
        lo = g * (per // 4)

        def pack(i):
            b = 4 * i
            for t in range(tiles):
                for side, X in ((0, xc), (1, 1)):
                    lanes = [
                        jnp.where(even_lane, cf[b + k, X, t], cf[b + k + 1, X, t]) for k in (0, 2)
                    ]
                    cxs[which, side, i, t] = jnp.where(even_row, lanes[0], lanes[1])
                for side, j in ((0, ROWS - 1), (1, 0)):
                    vs = [
                        view[pl.ds((((level * bands + b + k) * (xc + 2) + 1) * tiles + t) * ROWS + j, xc, stride=tiles * ROWS), :]
                        for k in range(4)
                    ]
                    ev = even_lane[:xc]
                    cys[which, side, i, t, 0:xc] = jnp.where(ev, vs[0], vs[1])
                    cys[which, side, i, t, xc : 2 * xc] = jnp.where(ev, vs[2], vs[3])

        loop(lo, lo + per // 4, pack)

        def pack_z(i):
            packed = jnp.zeros((ROWS, LANES), jnp.float32)
            for k in range(zper):
                for X in range(xc):
                    off = 4 * (k * xc + X)
                    w = jnp.where(low_half, cf[zper * i + k, 1 + X, 0], cf[zper * i + k, 1 + X, tiles - 1])
                    packed = jnp.where(lane // 4 == off // 4, roll(w, 2 + off, 1), packed)
            czs[which, i] = packed

        loop(g * (per // zper), (g + 1) * (per // zper), pack_z)
        start(coarse_copies(which, g))

    def spread_lanes(p):
        return (
            jnp.where(even_lane, p, roll(p, 1, 1)),
            jnp.where(even_lane, roll(p, -1, 1), p),
        )

    def coarse_unpack(which, level, g):
        cf = coarse.at[level]
        view = flat(hcy)
        lo = g * (per // 4)

        def unpack(i):
            b = 4 * i
            for t in range(tiles):
                for side, X in ((0, 0), (1, xc + 1)):
                    p = cxr[which, side, i, t]
                    top = jnp.where(even_row, p, roll(p, 1, 0))
                    low = jnp.where(even_row, roll(p, -1, 0), p)
                    for k, v in enumerate(spread_lanes(top) + spread_lanes(low)):
                        cf[b + k, X, t] = v
                for side, j in ((0, ROWS - 2), (1, 0)):
                    first, second = spread_lanes(cyr[which, side, i, t])
                    for k, v in enumerate((first[:xc], second[:xc], first[xc:], second[xc:])):
                        base = ((b + k) * xc * tiles + t) * ROWS + j
                        for dup in range(2):
                            view[pl.ds(base + dup, xc, stride=tiles * ROWS), :] = v

        loop(lo, lo + per // 4, unpack)

    def coarse_loop(which, g, f):
        def bundle(i):
            zp = czr[which, 0, i]
            if nz > 2:
                zp = jnp.where(first_of_four, zp, czr[which, 1, i])
            for k in range(zper):
                f(zper * i + k, lambda X, k=k: roll(zp, -(4 * (k * xc + X) + 2), 1))

        loop(g * (per // zper), (g + 1) * (per // zper), bundle)

    def sweep(which, level, g):
        coarse_unpack(which, level, g)

        def one(b, hz):
            for X in range(xc):
                vs = [coarse[level, b, 1 + X, t] for t in range(tiles)]
                z = shifted_z(vs, hz(X), 2)
                for t in range(tiles):
                    s = coarse[level, b, X, t] + coarse[level, b, 2 + X, t] + shifted_y(vs[t], hcy[b, X, t], 2) + z[t]
                    rhs = coarse[0, b, 1 + X, t]
                    coarse[level + 1, b, 1 + X, t] = (
                        (1.0 - WEIGHT) * vs[t] + (0.125 * WEIGHT / COARSE_DIAG) * s + rhs
                    )

        coarse_loop(which, g, one)

    def prolong(which, level, g, use):
        coarse_unpack(which, level, g)

        def one(b, hz):
            for X in range(xc):
                vs = [coarse[level, b, 1 + X, t] for t in range(tiles)]
                z = shifted_z(vs, hz(X), 1)
                for t in range(tiles):
                    s = shifted_y(vs[t], hcy[b, X, t], 1) + z[t] + vs[t]
                    for x, other in ((2 * X, X), (2 * X + 1, 2 + X)):
                        total = s + coarse[level, b, other, t]
                        kr = (1.0 - WEIGHT) * (res[b, 2 + x, t] + vs[t] + rem[b, x, t]) + (
                            0.5 * WEIGHT / 4.0
                        ) * total
                        use(b, x, t, kr)

        coarse_loop(which, g, one)

    def apply_one(g, b):
        norm, energy = [], []

        def use(x, vs, outs):
            for t in range(tiles):
                app[b, 2 + x, t] = outs[t]
                norm.append(vs[t] * vs[t])
                energy.append(vs[t] * outs[t])

        hamiltonian(orb, 0, b, use)
        acc[0, g, pl.ds(b - g * per, 1), :] = rowsum(norm)
        acc[0, g, pl.ds(b - g * per + per, 1), :] = rowsum(energy)

    def prepare_first(b):
        e = get(0, b)
        for x in range(1, xs + 3):
            for t in range(tiles):
                res[b, x, t] = app[b, x, t] - e * orb[b, x, t]

        def ry(s, j, t):
            return fyr[1][s, b, 0, t] - e * fyr[0][s, b, 1 - s, t]

        restrict(b, ry, z_packed(fzr[1], b) - e * z_packed(fzr[0], b))

    def use_first(b, x, t, kr):
        cor[b, 2 + x, t] = kr

    def respond_one(g, b):
        e = get(0, b)
        dots = [None] * NDOTS

        def use(x, vs, outs):
            for t in range(tiles):
                c, o, r = vs[t], orb[b, 2 + x, t], res[b, 2 + x, t]
                p = outs[t] - e * c
                rsp[b, 2 + x, t] = p
                for q, (u, v) in enumerate(((r, p), (p, p), (o, c), (c, c), (p, o), (p, c), (r, o), (r, c))):
                    w = u * v
                    dots[q] = w if dots[q] is None else dots[q] + w

        hamiltonian(cor, 2, b, use)
        for q in range(NDOTS):
            acc[1, g, pl.ds(b - g * per + q * per, 1), :] = rowsum([dots[q]])

    def prepare_second(b):
        e, ml, mc, mcl = get(0, b), get(2, b), get(3, b), get(4, b)

        def mixed(r, p, o, c):
            return r + ml * p - mc * o - mcl * c

        for x in range(1, xs + 3):
            for t in range(tiles):
                res[b, x, t] = mixed(res[b, x, t], rsp[b, x, t], orb[b, x, t], cor[b, x, t])

        def ry(s, j, t):
            o = fyr[0][s, b, 1 - s, t]
            r = fyr[1][s, b, 0, t] - e * o
            return mixed(r, fyr[3][s, b, 0, t], o, fyr[2][s, b, 1 - s, t])

        oz = z_packed(fzr[0], b)
        rz = z_packed(fzr[1], b) - e * oz
        restrict(b, ry, mixed(rz, z_packed(fzr[3], b), oz, z_packed(fzr[2], b)))

    def use_second(b, x, t, kr):
        out[b, x, :, t * LANES : (t + 1) * LANES] = (
            orb[b, 2 + x, t] + get(2, b) * cor[b, 2 + x, t] + get(1, b) * kr
        )

    def coarse_solve(base, use, then):
        for s in range(COARSE_SWEEPS):

            def step(g, s=s):
                wait(coarse_copies(base + s, g))
                if s < COARSE_SWEEPS - 1:
                    sweep(base + s, s, g)
                    coarse_send(base + s + 1, s + 1, g)
                else:
                    prolong(base + s, s, g, use)
                    then(g)

            loop(0, GROUPS, step)

    def begin(g):
        wait(load_copies(g))
        fine_send(orb, 0, 2, g)

    def first_hamiltonian(g):
        wait(fine_copies(orb, 0, 2, g))
        loop(g * per, (g + 1) * per, functools.partial(apply_one, g))
        reduce_start(0, g, 2)
        fine_send(app, 1, 1, g)

    def first_residual(g):
        norm_orbitals, first_energy = reduce_finish(0, g, 2)
        energy = first_energy / (norm_orbitals + EPSILON)
        for i, v in enumerate((norm_orbitals, first_energy, energy)):
            keep[i, g] = v
        put(0, g, energy)
        wait(fine_copies(app, 1, 1, g))
        loop(g * per, (g + 1) * per, prepare_first)
        coarse_send(0, 0, g)

    def second_hamiltonian(g):
        wait(fine_copies(cor, 2, 2, g))
        loop(g * per, (g + 1) * per, functools.partial(respond_one, g))
        reduce_start(1, g, NDOTS)
        fine_send(rsp, 3, 1, g)

    def second_residual(g):
        norm_orbitals, first_energy, energy = (keep[i, g] for i in range(3))
        rp, pp, oc, cc, po, pc, ro, rc = reduce_finish(1, g, NDOTS)
        lam = -rp / (pp + EPSILON)
        trial_norm = norm_orbitals + 2.0 * lam * oc + lam * lam * cc
        trial_sum = (
            first_energy + lam * ((po + energy * oc) + (rc + energy * oc)) + lam * lam * (pc + energy * cc)
        )
        trial = trial_sum / (trial_norm + EPSILON)
        energies[pl.ds(g, 1), :] = trial[0:1]
        change = trial - energy
        projected = lam * rp - change * (ro + lam * rc)
        cross = po + lam * pc
        change_norm = lam * lam * pp - 2.0 * lam * change * cross + change * change * trial_norm
        mix = -projected / (change_norm + EPSILON)
        put(1, g, lam)
        put(2, g, mix * lam)
        put(3, g, mix * change)
        put(4, g, mix * change * lam)
        wait(fine_copies(rsp, 3, 1, g))
        loop(g * per, (g + 1) * per, prepare_second)
        coarse_send(COARSE_SWEEPS, 0, g)

    pl.semaphore_wait(barrier, devices - 1)
    loop(0, GROUPS, begin)
    pot_load.wait()
    loop(0, GROUPS, first_hamiltonian)
    loop(0, GROUPS, first_residual)
    coarse_solve(0, use_first, lambda g: fine_send(cor, 2, 2, g))
    loop(0, GROUPS, second_hamiltonian)
    loop(0, GROUPS, second_residual)
    coarse_solve(COARSE_SWEEPS, use_second, lambda g: None)


def solution(mesh):
    sizes = tuple(mesh.shape[a] for a in AXES)

    def body(orbitals, potential):
        bands, xs, ys, zs = orbitals.shape
        tiles = zs // LANES
        tile = (ROWS, LANES)
        vmem = lambda *s: pltpu.VMEM(s + tile, jnp.float32)
        field = vmem(bands, xs + 4, tiles)
        exchanges = 4 + 2 * COARSE_SWEEPS
        faces = (2 * COARSE_SWEEPS, 2, bands // 4, tiles)
        devices = sizes[0] * sizes[1] * sizes[2]
        per = bands // GROUPS
        zbundles = bands // min(per, 8)

        def call(*refs):
            refs = list(refs)
            head, rest = refs[:4], refs[4:]
            fields, rest = rest[:7], rest[7:]
            fys, rest = rest[:4], rest[4:]
            fyr, rest = rest[:4], rest[4:]
            fzs, rest = rest[:4], rest[4:]
            fzr, rest = rest[:4], rest[4:]
            kernel(sizes, *head, *fields, fys, fyr, fzs, fzr, *rest)

        depths = (2, 1, 2, 1)
        updated, trial = pl.pallas_call(
            call,
            out_shape=(
                jax.ShapeDtypeStruct(orbitals.shape, jnp.float32),
                jax.ShapeDtypeStruct(tile, jnp.float32),
            ),
            in_specs=[
                pl.BlockSpec(memory_space=pltpu.HBM),
                pl.BlockSpec(memory_space=pltpu.HBM),
            ],
            out_specs=(
                pl.BlockSpec(memory_space=pltpu.VMEM),
                pl.BlockSpec(memory_space=pltpu.VMEM),
            ),
            scratch_shapes=[field] * 5
            + [vmem(bands, xs, tiles), vmem(COARSE_SWEEPS, bands, xs // 2 + 2, tiles)]
            + [vmem(2, bands, d, tiles) for d in depths]
            + [vmem(2, bands, d, tiles) for d in depths]
            + [vmem(bands) for d in depths]
            + [vmem(2, bands) for d in depths]
            + [
                vmem(bands, xs, tiles),
                vmem(*faces),
                vmem(*faces),
                vmem(*faces),
                vmem(*faces),
                vmem(2 * COARSE_SWEEPS, zbundles),
                vmem(2 * COARSE_SWEEPS, 2, zbundles),
                vmem(bands, xs // 2, tiles),
                pltpu.VMEM((2, GROUPS, NDOTS * per, LANES), jnp.float32),
                pltpu.VMEM((5, bands, LANES), jnp.float32),
                vmem(3, GROUPS),
                pltpu.VMEM((2 * GROUPS, devices, 1, LANES), jnp.float32),
                pltpu.VMEM(potential.shape, jnp.float32),
                pltpu.SemaphoreType.DMA((GROUPS + 1, tiles)),
                pltpu.SemaphoreType.DMA((exchanges * GROUPS, 6)),
                pltpu.SemaphoreType.DMA((exchanges * GROUPS, 6)),
                pltpu.SemaphoreType.DMA((2 * GROUPS,)),
                pltpu.SemaphoreType.DMA((2 * GROUPS,)),
            ],
            compiler_params=pltpu.CompilerParams(
                collective_id=0, has_side_effects=True, vmem_limit_bytes=48 * 1024 * 1024
            ),
        )(orbitals, potential)
        return updated, trial[:GROUPS, :per].reshape(bands)

    return jax.shard_map(
        body,
        mesh=mesh,
        in_specs=(P(None, "gx", "gy", "gz"), P("gx", "gy", "gz")),
        out_specs=(P(None, "gx", "gy", "gz"), P()),
        check_vma=False,
    )
```

```python
import functools

import jax
import jax.numpy as jnp
from jax import lax
from jax.experimental import pallas as pl
from jax.experimental.pallas import tpu as pltpu
from jax.sharding import PartitionSpec as P

COARSE_SWEEPS = 4
QUAD = 4
WEIGHT = 0.8
COARSE_DIAG = 1.75
EPSILON = 1e-06
LANES = 128
ROWS = 8
GROUPS = 4
AXES = ("gx", "gy", "gz")
MESH = pl.DeviceIdType.MESH
NDOTS = 8


def kernel(sizes, orb_hbm, pot_hbm, out, energies, *scratch):
    (
        orb, app, res, cor, rsp, rem, coarse,
        fys, fyr, fzs, fzr, hy, beside, czs, czr, czm, dup, duph, dupz,
        acc, scal, keep, red, pot, load_sem, send_sem, recv_sem, rsend, rrecv,
    ) = scratch
    nx, ny, nz = sizes
    bands, xs = orb_hbm.shape[0], orb_hbm.shape[1]
    tiles = orb_hbm.shape[3] // LANES
    xc = xs // 2
    per = bands // GROUPS
    devices = nx * ny * nz
    me = [lax.axis_index(a) for a in AXES]
    right = [lax.rem(m + 1, n) for m, n in zip(me, sizes)]
    left = [lax.rem(m + n - 1, n) for m, n in zip(me, sizes)]

    here = (me[0] * ny + me[1]) * nz + me[2]

    def start(copies):
        for c in copies:
            c.start()

    def wait(copies):
        for c in copies:
            c.wait()

    pot_load = pltpu.make_async_copy(pot_hbm, pot, load_sem.at[GROUPS, 0])

    def load_copies(g):
        part = pl.ds(g * per, per)
        return [
            pltpu.make_async_copy(
                orb_hbm.at[part, :, :, pl.ds(t * LANES, LANES)],
                orb.at[part, pl.ds(2, xs), t],
                load_sem.at[g, t],
            )
            for t in range(tiles)
        ]

    for g in range(GROUPS):
        start(load_copies(g))
    pot_load.start()

    def wrap(k, d):
        return lax.rem(me[k] + d, sizes[k])

    def every_peer(f):
        if devices <= 64:
            xyz = [[me[k]] + [wrap(k, d) for d in range(1, sizes[k])] for k in range(3)]
            for d in range(1, devices):
                f((xyz[0][d // (ny * nz)], xyz[1][d // nz % ny], xyz[2][d % nz]))
        else:

            def step(d, carry):
                f((wrap(0, d // (ny * nz)), wrap(1, lax.rem(d // nz, ny)), wrap(2, lax.rem(d, nz))))
                return carry

            lax.fori_loop(1, devices, step, 0)

    barrier = pltpu.get_barrier_semaphore()
    every_peer(lambda to: pl.semaphore_signal(barrier, inc=1, device_id=to, device_id_type=MESH))

    row = lax.broadcasted_iota(jnp.int32, (ROWS, LANES), 0)
    lane = lax.broadcasted_iota(jnp.int32, (ROWS, LANES), 1)
    even_lane = lane % 2 == 0
    even_row = row % 2 == 0
    low_half = lane < LANES // 2
    first_of_four = lane % 4 < 2
    first_of_eight = lane % 8 < 4
    top_half = row < ROWS // 2

    def roll(v, k, axis):
        return pltpu.roll(v, k % v.shape[axis], axis)

    def flat(ref):
        n = 1
        for s in ref.shape[:-1]:
            n *= s
        return ref.reshape(n, LANES)

    def loop(lo, hi, f):
        def step(i, carry):
            f(i)
            return carry

        lax.fori_loop(lo, hi, step, 0)

    def remote(src, dst, slot, k, axis, target):
        return pltpu.make_async_remote_copy(
            src_ref=src,
            dst_ref=dst,
            send_sem=send_sem.at[slot, k],
            recv_sem=recv_sem.at[slot, k],
            device_id={axis: target},
            device_id_type=MESH,
        )

    def z_copies(src, dst_l, dst_r, slot):
        copies = [remote(src, dst_l, slot, 4, "gz", right[2])]
        if nz > 2:
            copies.append(remote(src, dst_r, slot, 5, "gz", left[2]))
        return copies

    def fine_copies(field, which, depth, g):
        slot = which * GROUPS + g
        part = pl.ds(g * per, per)
        ys, yr = fys[which], fyr[which]
        zs, zr = fzs[which], fzr[which]
        return [
            remote(field.at[part, pl.ds(2 + xs - depth, depth)], field.at[part, pl.ds(2 - depth, depth)], slot, 0, "gx", right[0]),
            remote(field.at[part, pl.ds(2, depth)], field.at[part, pl.ds(2 + xs, depth)], slot, 1, "gx", left[0]),
            remote(ys.at[0, part], yr.at[0, part], slot, 2, "gy", right[1]),
            remote(ys.at[1, part], yr.at[1, part], slot, 3, "gy", left[1]),
        ] + z_copies(zs.at[part], zr.at[0, part], zr.at[1, part], slot)

    def fine_send(field, which, depth, g):
        view = flat(field)
        span = field.shape[1]
        ys, zs = fys[which], fzs[which]

        def pack(b):
            for t in range(tiles):
                for j in range(depth):
                    base = ((b * span + 2) * tiles + t) * ROWS
                    ys[0, b, j, t] = view[pl.ds(base + ROWS - depth + j, xs, stride=tiles * ROWS), :]
                    ys[1, b, j, t] = view[pl.ds(base + j, xs, stride=tiles * ROWS), :]
            packed = jnp.zeros((ROWS, LANES), jnp.float32)
            for x in range(xs):
                w = jnp.where(low_half, field[b, 2 + x, 0], field[b, 2 + x, tiles - 1])
                packed = jnp.where(lane // 4 == x, roll(w, 2 + 4 * x, 1), packed)
            zs[b] = packed

        loop(g * per, (g + 1) * per, pack)
        start(fine_copies(field, which, depth, g))

    def z_packed(zr, b):
        if nz > 2:
            return jnp.where(first_of_four, zr[0, b], zr[1, b])
        return zr[0, b]

    def unpack_y(yr, b, depth):
        view = flat(hy)
        for t in range(tiles):
            for j in range(depth):
                base = (b * xs * tiles + t) * ROWS
                view[pl.ds(base + ROWS - depth + j, xs, stride=tiles * ROWS), :] = yr(0, j, t)
                view[pl.ds(base + j, xs, stride=tiles * ROWS), :] = yr(1, j, t)

    def shifted_y(v, h, k):
        up = roll(jnp.where(row >= ROWS - k, h, v), k, 0)
        down = roll(jnp.where(row < k, h, v), -k, 0)
        return up + down

    def shifted_z(vs, hz, k):
        before = [hz] + vs[:-1]
        after = vs[1:] + [hz]
        return [
            roll(jnp.where(lane >= LANES - k, p, v), k, 1) + roll(jnp.where(lane < k, n, v), -k, 1)
            for p, v, n in zip(before, vs, after)
        ]

    def hamiltonian(field, which, b, use):
        unpack_y(lambda s, j, t: fyr[which][s, b, j, t], b, 2)
        zp = z_packed(fzr[which], b)
        for x in range(xs):
            hz = roll(zp, -(4 * x + 2), 1)
            vs = [field[b, 2 + x, t] for t in range(tiles)]
            z1, z2 = shifted_z(vs, hz, 1), shifted_z(vs, hz, 2)
            outs = []
            for t in range(tiles):
                h = hy[b, x, t]
                near = field[b, 1 + x, t] + field[b, 3 + x, t] + shifted_y(vs[t], h, 1) + z1[t]
                far = field[b, x, t] + field[b, 4 + x, t] + shifted_y(vs[t], h, 2) + z2[t]
                potential = pot[x, :, t * LANES : (t + 1) * LANES]
                outs.append((potential + 3.75) * vs[t] - (2.0 / 3.0) * near + (1.0 / 24.0) * far)
            use(x, vs, outs)

    def rowsum(vs):
        return jnp.sum(functools.reduce(jnp.add, vs), axis=0, keepdims=True)

    def reduce_start(index, g, ndots):
        total = jnp.zeros((ROWS, LANES), jnp.float32)
        for i in range(ndots * per // ROWS):
            part = jnp.sum(acc[index, g, i * ROWS : (i + 1) * ROWS, :], axis=1, keepdims=True)
            total = jnp.where(lane == row + i * ROWS, part, total)
        k = index * GROUPS + g
        red[k, here] = jnp.sum(total, axis=0, keepdims=True)

        def send(to):
            pltpu.make_async_remote_copy(
                src_ref=red.at[k, here],
                dst_ref=red.at[k, here],
                send_sem=rsend.at[k],
                recv_sem=rrecv.at[k],
                device_id=to,
                device_id_type=MESH,
            ).start()

        every_peer(send)

    def reduce_finish(index, g, ndots):
        k = index * GROUPS + g
        rest = red.at[k, pl.ds(0, devices - 1)]
        pltpu.make_async_copy(rest, rest, rrecv.at[k]).wait()
        pltpu.make_async_copy(rest, rest, rsend.at[k]).wait()
        total = jnp.broadcast_to(jnp.sum(red[k], axis=0), (ROWS, LANES))
        return [total if q == 0 else roll(total, -q * per, 1) for q in range(ndots)]

    def put(k, g, values):
        for b in range(per):
            scal[k, pl.ds(g * per + b, 1), :] = jnp.broadcast_to(values[0:1, b : b + 1], (1, LANES))

    def get(k, b):
        return scal[k, pl.ds(b, 1), :]

    def restrict(b, ry, rz):
        k = lax.rem(b, QUAD)
        unpack_y(ry, b, 1)
        for X in range(xc):
            pair = [None] * tiles
            for x in (2 * X, 2 * X + 1):
                hz = roll(rz, -(4 * x + 2), 1)
                vs = [res[b, 2 + x, t] for t in range(tiles)]
                z1 = shifted_z(vs, hz, 1)
                for t in range(tiles):
                    s = res[b, 1 + x, t] + res[b, 3 + x, t] + shifted_y(vs[t], hy[b, x, t], 1) + z1[t]
                    m = (1.0 - WEIGHT) * vs[t] + (0.5 * WEIGHT / 4.0) * s
                    rem[b, x, t] = m
                    pair[t] = m if pair[t] is None else pair[t] + m
            for t in range(tiles):
                s = pair[t]
                s = s + jnp.where(even_row, roll(s, -1, 0), roll(s, 1, 0))
                s = s + jnp.where(even_lane, roll(s, -1, 1), roll(s, 1, 1))
                dup[k, 1 + X, t] = s * (0.125 * WEIGHT / COARSE_DIAG)

    def coarse_pack(level, g):
        for X in range(xc):
            for t in range(tiles):
                lanes = [jnp.where(even_lane, dup[k, 1 + X, t], dup[k + 1, 1 + X, t]) for k in (0, 2)]
                coarse[level, g, 2 + X, t] = jnp.where(even_row, lanes[0], lanes[1])

    def coarse_copies(level, w, g):
        slot = (4 + w) * GROUPS + g
        own, side = coarse.at[level, g], beside.at[level, g]
        low, high = pl.ds(0, ROWS // 2), pl.ds(ROWS // 2, ROWS // 2)
        inner, last, first = pl.ds(2, xc), 1 + xc, 2
        right_x, left_x = {"gx": right[0]}, {"gx": left[0]}
        right_y, left_y = {"gy": right[1]}, {"gy": left[1]}
        moves = [
            (own.at[pl.ds(xc, 2)], own.at[pl.ds(0, 2)], right_x),
            (own.at[pl.ds(2, 2)], own.at[pl.ds(2 + xc, 2)], left_x),
            (own.at[inner, :, high], side.at[pl.ds(1, xc), :, high], right_y),
            (own.at[inner, :, low], side.at[pl.ds(1, xc), :, low], left_y),
            (own.at[last, :, high], side.at[0, :, high], right_x | right_y),
            (own.at[last, :, low], side.at[0, :, low], right_x | left_y),
            (own.at[first, :, high], side.at[1 + xc, :, high], left_x | right_y),
            (own.at[first, :, low], side.at[1 + xc, :, low], left_x | left_y),
        ]
        for end, z in enumerate((right[2], left[2])[: 1 if nz == 2 else 2]):
            for i, to in enumerate(({}, right_x, left_x, right_y, left_y)):
                moves.append((czs.at[w, g], czr.at[w, i, end, g], to | {"gz": z}))
        return [
            pltpu.make_async_remote_copy(
                src_ref=src,
                dst_ref=dst,
                send_sem=send_sem.at[slot, k],
                recv_sem=recv_sem.at[slot, k],
                device_id=to,
                device_id_type=MESH,
            )
            for k, (src, dst, to) in enumerate(moves)
        ]

    def coarse_send(level, w, g):
        packed = jnp.zeros((ROWS, LANES), jnp.float32)
        for X in range(xc):
            v = jnp.where(low_half, coarse[level, g, 2 + X, 0], coarse[level, g, 2 + X, tiles - 1])
            packed = jnp.where(lane // 8 == X, roll(v, 8 * X + 4, 1), packed)
        czs[w, g] = packed
        start(coarse_copies(level, w, g))

    def z_edges(w, i, g):
        if nz > 2:
            return jnp.where(first_of_eight, czr[w, i, 0, g], czr[w, i, 1, g])
        return czr[w, i, 0, g]

    def z_halo(packed, X):
        return roll(packed, -(8 * X + 4), 1)

    def update(v, s, rhs):
        return (1.0 - WEIGHT) * v + (0.125 * WEIGHT / COARSE_DIAG) * s + rhs

    def sweep_plane(zero, level, g, X, hz):
        vs = [coarse[level, g, 2 + X, t] for t in range(tiles)]
        z = shifted_z(vs, hz, 2)
        for t in range(tiles):
            s = coarse[level, g, 1 + X, t] + coarse[level, g, 3 + X, t]
            s = s + shifted_y(vs[t], beside[level, g, 1 + X, t], 2) + z[t]
            coarse[level + 1, g, 2 + X, t] = update(vs[t], s, coarse[zero, g, 2 + X, t])

    def sweep_wide(zero, level, w, g):
        zc, from_left, from_right, from_below, from_above = (z_edges(w, i, g) for i in range(5))
        zs, zy = czs[w, g], jnp.where(top_half, from_above, from_below)
        for X in range(-1, xc + 1):
            if X < 0:
                hz = z_halo(from_left, xc - 1)
            elif X == xc:
                hz = z_halo(from_right, 0)
            else:
                hz = z_halo(zc, X)
            sweep_plane(zero, level, g, X, hz)
        for X in range(xc):
            hs = [beside[level, g, 1 + X, t] for t in range(tiles)]
            z = shifted_z(hs, z_halo(zy, X), 2)
            for t in range(tiles):
                h, v = hs[t], coarse[level, g, 2 + X, t]
                y = jnp.where(top_half, roll(h, -2, 0) + roll(v, 2, 0), roll(h, 2, 0) + roll(v, -2, 0))
                s = beside[level, g, X, t] + beside[level, g, 2 + X, t] + y + z[t]
                beside[level + 1, g, 1 + X, t] = update(h, s, beside[zero, g, 1 + X, t])
        edge = 8 * (xc - 1)
        s = jnp.where(lane < 8, roll(from_left, -edge, 1), roll(zc, 8, 1))
        s = s + jnp.where(lane >= edge, roll(from_right, edge, 1), roll(zc, -8, 1))
        s = s + shifted_y(zc, zy, 2)
        s = s + jnp.where(
            first_of_eight, roll(zc, 2, 1) + roll(zs, -2, 1), roll(zc, -2, 1) + roll(zs, 2, 1)
        )
        czm[w, g] = update(zc, s, z_edges(w // 2 * 2, 0, g))

    def sweep_own(zero, level, w, g):
        zc = czm[w, g]
        for X in range(xc):
            sweep_plane(zero, level, g, X, z_halo(zc, X))

    def spread(p):
        out = []
        for v in (jnp.where(even_row, p, roll(p, 1, 0)), jnp.where(even_row, roll(p, -1, 0), p)):
            out.append(jnp.where(even_lane, v, roll(v, 1, 1)))
            out.append(jnp.where(even_lane, roll(v, -1, 1), v))
        return out

    def prolong(level, w, g, use):
        zc = czm[w, g]
        for X in range(xc + 2):
            for t in range(tiles):
                for k, v in enumerate(spread(coarse[level, g, 1 + X, t])):
                    dup[k, X, t] = v
        for X in range(xc):
            for t in range(tiles):
                for k, v in enumerate(spread(beside[level, g, 1 + X, t])):
                    duph[k, X, t] = v
            for k, v in enumerate(spread(z_halo(zc, X))):
                dupz[k, X] = v

        def one(b):
            k = lax.rem(b, QUAD)
            for X in range(xc):
                vs = [dup[k, 1 + X, t] for t in range(tiles)]
                z = shifted_z(vs, dupz[k, X], 1)
                for t in range(tiles):
                    s = shifted_y(vs[t], duph[k, X, t], 1) + z[t] + vs[t]
                    for x, other in ((2 * X, X), (2 * X + 1, 2 + X)):
                        total = s + dup[k, other, t]
                        kr = (1.0 - WEIGHT) * (res[b, 2 + x, t] + vs[t] + rem[b, x, t]) + (
                            0.5 * WEIGHT / 4.0
                        ) * total
                        use(b, x, t, kr)

        loop(g * per, (g + 1) * per, one)

    def apply_one(g, b):
        norm, energy = [], []

        def use(x, vs, outs):
            for t in range(tiles):
                app[b, 2 + x, t] = outs[t]
                norm.append(vs[t] * vs[t])
                energy.append(vs[t] * outs[t])

        hamiltonian(orb, 0, b, use)
        acc[0, g, pl.ds(b - g * per, 1), :] = rowsum(norm)
        acc[0, g, pl.ds(b - g * per + per, 1), :] = rowsum(energy)

    def prepare_first(b):
        e = get(0, b)
        for x in range(1, xs + 3):
            for t in range(tiles):
                res[b, x, t] = app[b, x, t] - e * orb[b, x, t]

        def ry(s, j, t):
            return fyr[1][s, b, 0, t] - e * fyr[0][s, b, 1 - s, t]

        restrict(b, ry, z_packed(fzr[1], b) - e * z_packed(fzr[0], b))

    def use_first(b, x, t, kr):
        cor[b, 2 + x, t] = kr

    def respond_one(g, b):
        e = get(0, b)
        dots = [None] * NDOTS

        def use(x, vs, outs):
            for t in range(tiles):
                c, o, r = vs[t], orb[b, 2 + x, t], res[b, 2 + x, t]
                p = outs[t] - e * c
                rsp[b, 2 + x, t] = p
                for q, (u, v) in enumerate(((r, p), (p, p), (o, c), (c, c), (p, o), (p, c), (r, o), (r, c))):
                    w = u * v
                    dots[q] = w if dots[q] is None else dots[q] + w

        hamiltonian(cor, 2, b, use)
        for q in range(NDOTS):
            acc[1, g, pl.ds(b - g * per + q * per, 1), :] = rowsum([dots[q]])

    def prepare_second(b):
        e, ml, mc, mcl = get(0, b), get(2, b), get(3, b), get(4, b)

        def mixed(r, p, o, c):
            return r + ml * p - mc * o - mcl * c

        for x in range(1, xs + 3):
            for t in range(tiles):
                res[b, x, t] = mixed(res[b, x, t], rsp[b, x, t], orb[b, x, t], cor[b, x, t])

        def ry(s, j, t):
            o = fyr[0][s, b, 1 - s, t]
            r = fyr[1][s, b, 0, t] - e * o
            return mixed(r, fyr[3][s, b, 0, t], o, fyr[2][s, b, 1 - s, t])

        oz = z_packed(fzr[0], b)
        rz = z_packed(fzr[1], b) - e * oz
        restrict(b, ry, mixed(rz, z_packed(fzr[3], b), oz, z_packed(fzr[2], b)))

    def use_second(b, x, t, kr):
        out[b, x, :, t * LANES : (t + 1) * LANES] = (
            orb[b, 2 + x, t] + get(2, b) * cor[b, 2 + x, t] + get(1, b) * kr
        )

    def coarse_begin(turn, g):
        coarse_pack(turn * COARSE_SWEEPS, g)
        coarse_send(turn * COARSE_SWEEPS, 2 * turn, g)

    def coarse_solve(turn, use, then):
        zero = turn * COARSE_SWEEPS
        w = 2 * turn

        def middle(g):
            wait(coarse_copies(zero, w, g))
            sweep_wide(zero, zero, w, g)
            sweep_own(zero, zero + 1, w, g)
            coarse_send(zero + 2, w + 1, g)

        def finish(g):
            wait(coarse_copies(zero + 2, w + 1, g))
            sweep_wide(zero, zero + 2, w + 1, g)
            prolong(zero + 3, w + 1, g, use)
            then(g)

        loop(0, GROUPS, middle)
        loop(0, GROUPS, finish)

    def begin(g):
        wait(load_copies(g))
        fine_send(orb, 0, 2, g)

    def first_hamiltonian(g):
        wait(fine_copies(orb, 0, 2, g))
        loop(g * per, (g + 1) * per, functools.partial(apply_one, g))
        reduce_start(0, g, 2)
        fine_send(app, 1, 1, g)

    def first_residual(g):
        norm_orbitals, first_energy = reduce_finish(0, g, 2)
        energy = first_energy / (norm_orbitals + EPSILON)
        for i, v in enumerate((norm_orbitals, first_energy, energy)):
            keep[i, g] = v
        put(0, g, energy)
        wait(fine_copies(app, 1, 1, g))
        loop(g * per, (g + 1) * per, prepare_first)
        coarse_begin(0, g)

    def second_hamiltonian(g):
        wait(fine_copies(cor, 2, 2, g))
        loop(g * per, (g + 1) * per, functools.partial(respond_one, g))
        reduce_start(1, g, NDOTS)
        fine_send(rsp, 3, 1, g)

    def second_residual(g):
        norm_orbitals, first_energy, energy = (keep[i, g] for i in range(3))
        rp, pp, oc, cc, po, pc, ro, rc = reduce_finish(1, g, NDOTS)
        lam = -rp / (pp + EPSILON)
        trial_norm = norm_orbitals + 2.0 * lam * oc + lam * lam * cc
        trial_sum = (
            first_energy + lam * ((po + energy * oc) + (rc + energy * oc)) + lam * lam * (pc + energy * cc)
        )
        trial = trial_sum / (trial_norm + EPSILON)
        energies[pl.ds(g, 1), :] = trial[0:1]
        change = trial - energy
        projected = lam * rp - change * (ro + lam * rc)
        cross = po + lam * pc
        change_norm = lam * lam * pp - 2.0 * lam * change * cross + change * change * trial_norm
        mix = -projected / (change_norm + EPSILON)
        put(1, g, lam)
        put(2, g, mix * lam)
        put(3, g, mix * change)
        put(4, g, mix * change * lam)
        wait(fine_copies(rsp, 3, 1, g))
        loop(g * per, (g + 1) * per, prepare_second)
        coarse_begin(1, g)

    pl.semaphore_wait(barrier, devices - 1)
    loop(0, GROUPS, begin)
    pot_load.wait()
    loop(0, GROUPS, first_hamiltonian)
    loop(0, GROUPS, first_residual)
    coarse_solve(0, use_first, lambda g: fine_send(cor, 2, 2, g))
    loop(0, GROUPS, second_hamiltonian)
    loop(0, GROUPS, second_residual)
    coarse_solve(1, use_second, lambda g: None)


def solution(mesh):
    sizes = tuple(mesh.shape[a] for a in AXES)

    def body(orbitals, potential):
        bands, xs, ys, zs = orbitals.shape
        tiles = zs // LANES
        tile = (ROWS, LANES)
        vmem = lambda *s: pltpu.VMEM(s + tile, jnp.float32)
        field = vmem(bands, xs + 4, tiles)
        exchanges = 8
        assert bands == QUAD * GROUPS
        devices = sizes[0] * sizes[1] * sizes[2]
        per = bands // GROUPS

        def call(*refs):
            refs = list(refs)
            head, rest = refs[:4], refs[4:]
            fields, rest = rest[:7], rest[7:]
            fys, rest = rest[:4], rest[4:]
            fyr, rest = rest[:4], rest[4:]
            fzs, rest = rest[:4], rest[4:]
            fzr, rest = rest[:4], rest[4:]
            kernel(sizes, *head, *fields, fys, fyr, fzs, fzr, *rest)

        depths = (2, 1, 2, 1)
        updated, trial = pl.pallas_call(
            call,
            out_shape=(
                jax.ShapeDtypeStruct(orbitals.shape, jnp.float32),
                jax.ShapeDtypeStruct(tile, jnp.float32),
            ),
            in_specs=[
                pl.BlockSpec(memory_space=pltpu.HBM),
                pl.BlockSpec(memory_space=pltpu.HBM),
            ],
            out_specs=(
                pl.BlockSpec(memory_space=pltpu.VMEM),
                pl.BlockSpec(memory_space=pltpu.VMEM),
            ),
            scratch_shapes=[field] * 5
            + [vmem(bands, xs, tiles), vmem(2 * COARSE_SWEEPS, GROUPS, xs // 2 + 4, tiles)]
            + [vmem(2, bands, d, tiles) for d in depths]
            + [vmem(2, bands, d, tiles) for d in depths]
            + [vmem(bands) for d in depths]
            + [vmem(2, bands) for d in depths]
            + [
                vmem(bands, xs, tiles),
                vmem(2 * COARSE_SWEEPS, GROUPS, xs // 2 + 2, tiles),
                vmem(4, GROUPS),
                vmem(4, 5, 2, GROUPS),
                vmem(4, GROUPS),
                vmem(QUAD, xs // 2 + 2, tiles),
                vmem(QUAD, xs // 2, tiles),
                vmem(QUAD, xs // 2),
                pltpu.VMEM((2, GROUPS, NDOTS * per, LANES), jnp.float32),
                pltpu.VMEM((5, bands, LANES), jnp.float32),
                vmem(3, GROUPS),
                pltpu.VMEM((2 * GROUPS, devices, 1, LANES), jnp.float32),
                pltpu.VMEM(potential.shape, jnp.float32),
                pltpu.SemaphoreType.DMA((GROUPS + 1, tiles)),
                pltpu.SemaphoreType.DMA((exchanges * GROUPS, 18)),
                pltpu.SemaphoreType.DMA((exchanges * GROUPS, 18)),
                pltpu.SemaphoreType.DMA((2 * GROUPS,)),
                pltpu.SemaphoreType.DMA((2 * GROUPS,)),
            ],
            compiler_params=pltpu.CompilerParams(
                collective_id=0, has_side_effects=True, vmem_limit_bytes=48 * 1024 * 1024
            ),
        )(orbitals, potential)
        return updated, trial[:GROUPS, :per].reshape(bands)

    return jax.shard_map(
        body,
        mesh=mesh,
        in_specs=(P(None, "gx", "gy", "gz"), P("gx", "gy", "gz")),
        out_specs=(P(None, "gx", "gy", "gz"), P()),
        check_vma=False,
    )
```

```python
import functools

import jax
import jax.numpy as jnp
from jax import lax
from jax.experimental import pallas as pl
from jax.experimental.pallas import tpu as pltpu
from jax.sharding import PartitionSpec as P

COARSE_SWEEPS = 4
QUAD = 4
WEIGHT = 0.8
COARSE_DIAG = 1.75
EPSILON = 1e-06
LANES = 128
ROWS = 8
GROUPS = 4
AXES = ("gx", "gy", "gz")
MESH = pl.DeviceIdType.MESH
NDOTS = 8


def kernel(sizes, orb_hbm, pot_hbm, out, energies, *scratch):
    (
        orb, app, res, cor, rsp, rem, coarse,
        fys, fyr, fzs, fzr, hy, beside, czs, czr, czm, dup, duph, dupz,
        acc, scal, keep, red, pot, load_sem, send_sem, recv_sem, rsend, rrecv, greet_y, greet_z,
    ) = scratch
    nx, ny, nz = sizes
    bands, xs = orb_hbm.shape[0], orb_hbm.shape[1]
    tiles = orb_hbm.shape[3] // LANES
    xc = xs // 2
    per = bands // GROUPS
    devices = nx * ny * nz
    me = [lax.axis_index(a) for a in AXES]
    right = [lax.rem(m + 1, n) for m, n in zip(me, sizes)]
    left = [lax.rem(m + n - 1, n) for m, n in zip(me, sizes)]

    here = (me[0] * ny + me[1]) * nz + me[2]

    def start(copies):
        for c in copies:
            c.start()

    def wait(copies):
        for c in copies:
            c.wait()

    pot_load = pltpu.make_async_copy(pot_hbm, pot, load_sem.at[GROUPS, 0])

    def load_copies(g):
        part = pl.ds(g * per, per)
        return [
            pltpu.make_async_copy(
                orb_hbm.at[part, :, :, pl.ds(t * LANES, LANES)],
                orb.at[part, pl.ds(2, xs), t],
                load_sem.at[g, t],
            )
            for t in range(tiles)
        ]

    for g in range(GROUPS):
        start(load_copies(g))
    pot_load.start()

    def wrap(k, d):
        return lax.rem(me[k] + d, sizes[k])

    def every_peer(f):
        if devices <= 64:
            xyz = [[me[k]] + [wrap(k, d) for d in range(1, sizes[k])] for k in range(3)]
            for d in range(1, devices):
                f((xyz[0][d // (ny * nz)], xyz[1][d // nz % ny], xyz[2][d % nz]))
        else:

            def step(d, carry):
                f((wrap(0, d // (ny * nz)), wrap(1, lax.rem(d // nz, ny)), wrap(2, lax.rem(d, nz))))
                return carry

            lax.fori_loop(1, devices, step, 0)

    for level in (0, 2):
        for turn in range(2):
            for X in (0, 1 + xc):
                for g in range(GROUPS):
                    for t in range(tiles):
                        beside[turn * COARSE_SWEEPS + level, g, X, t] = jnp.zeros((ROWS, LANES), jnp.float32)

    def greet(semaphore, axes):
        for k in axes:
            for d in range(1, sizes[k]):
                pl.semaphore_signal(semaphore, inc=1, device_id={AXES[k]: wrap(k, d)}, device_id_type=MESH)

    def greeted(semaphore, axes):
        pl.semaphore_wait(semaphore, sum(sizes[k] - 1 for k in axes))

    barrier = pltpu.get_barrier_semaphore()
    greet(barrier, (0, 1, 2))

    row = lax.broadcasted_iota(jnp.int32, (ROWS, LANES), 0)
    lane = lax.broadcasted_iota(jnp.int32, (ROWS, LANES), 1)
    even_lane = lane % 2 == 0
    even_row = row % 2 == 0
    low_half = lane < LANES // 2
    first_of_four = lane % 4 < 2
    first_of_eight = lane % 8 < 4
    top_half = row < ROWS // 2

    z_ends = (right[2], left[2])[: 1 if nz == 2 else 2]

    def roll(v, k, axis):
        return pltpu.roll(v, k % v.shape[axis], axis)

    def flat(ref):
        n = 1
        for s in ref.shape[:-1]:
            n *= s
        return ref.reshape(n, LANES)

    def loop(lo, hi, f):
        def step(i, carry):
            f(i)
            return carry

        lax.fori_loop(lo, hi, step, 0)

    def remote(src, dst, turn, g, k, to):
        return pltpu.make_async_remote_copy(
            src_ref=src,
            dst_ref=dst,
            send_sem=send_sem.at[g, k],
            recv_sem=recv_sem.at[turn % 2, g, k],
            device_id=to,
            device_id_type=MESH,
        )

    def fine_copies(field, which, depth, g):
        part = pl.ds(g * per, per)
        ys, yr = fys[which], fyr[which]
        zs, zr = fzs[which], fzr[which]
        moves = [
            (field.at[part, pl.ds(2 + xs - depth, depth)], field.at[part, pl.ds(2 - depth, depth)], {"gx": right[0]}),
            (field.at[part, pl.ds(2, depth)], field.at[part, pl.ds(2 + xs, depth)], {"gx": left[0]}),
            (ys.at[0, part], yr.at[0, part], {"gy": right[1]}),
            (ys.at[1, part], yr.at[1, part], {"gy": left[1]}),
        ]
        for end, z in enumerate(z_ends):
            moves.append((zs.at[part], zr.at[end, part], {"gz": z}))
        return [remote(src, dst, which, g, k, to) for k, (src, dst, to) in enumerate(moves)]

    def fine_send(field, which, depth, g):
        view = flat(field)
        span = field.shape[1]
        ys, zs = fys[which], fzs[which]

        def pack(b):
            for t in range(tiles):
                for j in range(depth):
                    base = ((b * span + 2) * tiles + t) * ROWS
                    ys[0, b, j, t] = view[pl.ds(base + ROWS - depth + j, xs, stride=tiles * ROWS), :]
                    ys[1, b, j, t] = view[pl.ds(base + j, xs, stride=tiles * ROWS), :]
            packed = jnp.zeros((ROWS, LANES), jnp.float32)
            for x in range(xs):
                w = jnp.where(low_half, field[b, 2 + x, 0], field[b, 2 + x, tiles - 1])
                packed = jnp.where(lane // 4 == x, roll(w, 2 + 4 * x, 1), packed)
            zs[b] = packed

        loop(g * per, (g + 1) * per, pack)
        start(fine_copies(field, which, depth, g))

    def z_packed(zr, b):
        if nz > 2:
            return jnp.where(first_of_four, zr[0, b], zr[1, b])
        return zr[0, b]

    def unpack_y(yr, b, depth):
        view = flat(hy)
        for t in range(tiles):
            for j in range(depth):
                base = (b * xs * tiles + t) * ROWS
                view[pl.ds(base + ROWS - depth + j, xs, stride=tiles * ROWS), :] = yr(0, j, t)
                view[pl.ds(base + j, xs, stride=tiles * ROWS), :] = yr(1, j, t)

    def shifted_y(v, h, k):
        up = roll(jnp.where(row >= ROWS - k, h, v), k, 0)
        down = roll(jnp.where(row < k, h, v), -k, 0)
        return up + down

    def shifted_z(vs, hz, k):
        before = [hz] + vs[:-1]
        after = vs[1:] + [hz]
        return [
            roll(jnp.where(lane >= LANES - k, p, v), k, 1) + roll(jnp.where(lane < k, n, v), -k, 1)
            for p, v, n in zip(before, vs, after)
        ]

    def hamiltonian(field, which, b, use):
        unpack_y(lambda s, j, t: fyr[which][s, b, j, t], b, 2)
        zp = z_packed(fzr[which], b)
        for x in range(xs):
            hz = roll(zp, -(4 * x + 2), 1)
            vs = [field[b, 2 + x, t] for t in range(tiles)]
            z1, z2 = shifted_z(vs, hz, 1), shifted_z(vs, hz, 2)
            outs = []
            for t in range(tiles):
                h = hy[b, x, t]
                near = field[b, 1 + x, t] + field[b, 3 + x, t] + shifted_y(vs[t], h, 1) + z1[t]
                far = field[b, x, t] + field[b, 4 + x, t] + shifted_y(vs[t], h, 2) + z2[t]
                potential = pot[x, :, t * LANES : (t + 1) * LANES]
                outs.append((potential + 3.75) * vs[t] - (2.0 / 3.0) * near + (1.0 / 24.0) * far)
            use(x, vs, outs)

    def rowsum(vs):
        return jnp.sum(functools.reduce(jnp.add, vs), axis=0, keepdims=True)

    def reduce_start(index, g, ndots):
        total = jnp.zeros((ROWS, LANES), jnp.float32)
        for i in range(ndots * per // ROWS):
            part = jnp.sum(acc[index, g, i * ROWS : (i + 1) * ROWS, :], axis=1, keepdims=True)
            total = jnp.where(lane == row + i * ROWS, part, total)
        k = index * GROUPS + g
        red[k, here] = jnp.sum(total, axis=0, keepdims=True)

        def send(to):
            pltpu.make_async_remote_copy(
                src_ref=red.at[k, here],
                dst_ref=red.at[k, here],
                send_sem=rsend.at[k],
                recv_sem=rrecv.at[k],
                device_id=to,
                device_id_type=MESH,
            ).start()

        every_peer(send)

    def reduce_finish(index, g, ndots):
        k = index * GROUPS + g
        rest = red.at[k, pl.ds(0, devices - 1)]
        pltpu.make_async_copy(rest, rest, rrecv.at[k]).wait()
        pltpu.make_async_copy(rest, rest, rsend.at[k]).wait()
        total = jnp.broadcast_to(jnp.sum(red[k], axis=0), (ROWS, LANES))
        return [total if q == 0 else roll(total, -q * per, 1) for q in range(ndots)]

    def put(k, g, values):
        for b in range(per):
            scal[k, pl.ds(g * per + b, 1), :] = jnp.broadcast_to(values[0:1, b : b + 1], (1, LANES))

    def get(k, b):
        return scal[k, pl.ds(b, 1), :]

    def restrict(b, ry, rz):
        k = lax.rem(b, QUAD)
        unpack_y(ry, b, 1)
        for X in range(xc):
            pair = [None] * tiles
            for x in (2 * X, 2 * X + 1):
                hz = roll(rz, -(4 * x + 2), 1)
                vs = [res[b, 2 + x, t] for t in range(tiles)]
                z1 = shifted_z(vs, hz, 1)
                for t in range(tiles):
                    s = res[b, 1 + x, t] + res[b, 3 + x, t] + shifted_y(vs[t], hy[b, x, t], 1) + z1[t]
                    m = (1.0 - WEIGHT) * vs[t] + (0.5 * WEIGHT / 4.0) * s
                    rem[b, x, t] = m
                    pair[t] = m if pair[t] is None else pair[t] + m
            for t in range(tiles):
                s = pair[t]
                s = s + jnp.where(even_row, roll(s, -1, 0), roll(s, 1, 0))
                s = s + jnp.where(even_lane, roll(s, -1, 1), roll(s, 1, 1))
                dup[k, 1 + X, t] = s * (0.125 * WEIGHT / COARSE_DIAG)

    def coarse_pack(level, g):
        for X in range(xc):
            for t in range(tiles):
                lanes = [jnp.where(even_lane, dup[k, 1 + X, t], dup[k + 1, 1 + X, t]) for k in (0, 2)]
                coarse[level, g, 2 + X, t] = jnp.where(even_row, lanes[0], lanes[1])

    def coarse_copies(level, w, g):
        own, side = coarse.at[level, g], beside.at[level, g]
        low, high = pl.ds(0, ROWS // 2), pl.ds(ROWS // 2, ROWS // 2)
        top, bottom = pl.ds(0, 2), pl.ds(ROWS - 2, 2)
        inner, last, first = pl.ds(2, xc), 1 + xc, 2
        right_x, left_x = {"gx": right[0]}, {"gx": left[0]}
        right_y, left_y = {"gy": right[1]}, {"gy": left[1]}
        moves = [
            (own.at[pl.ds(xc, 2)], own.at[pl.ds(0, 2)], right_x),
            (own.at[pl.ds(2, 2)], own.at[pl.ds(2 + xc, 2)], left_x),
            (own.at[inner, :, high], side.at[pl.ds(1, xc), :, high], right_y),
            (own.at[inner, :, low], side.at[pl.ds(1, xc), :, low], left_y),
        ]
        for end, z in enumerate(z_ends):
            moves.append((czs.at[w, g], czr.at[w, 0, end, g], {"gz": z}))
        moves += [
            (own.at[last, :, bottom], side.at[0, :, bottom], right_x | right_y),
            (own.at[last, :, top], side.at[0, :, top], right_x | left_y),
            (own.at[first, :, bottom], side.at[1 + xc, :, bottom], left_x | right_y),
            (own.at[first, :, top], side.at[1 + xc, :, top], left_x | left_y),
        ]
        for end, z in enumerate(z_ends):
            for i, to in ((1, right_x), (2, left_x)):
                moves.append((czs.at[w, g], czr.at[w, i, end, g], to | {"gz": z}))
            for part, to in ((bottom, right_y), (top, left_y)):
                moves.append((czs.at[w, g, part], czr.at[w, 3, end, g, part], to | {"gz": z}))
        return [remote(src, dst, w, g, k, to) for k, (src, dst, to) in enumerate(moves)]

    def coarse_send(level, w, g):
        packed = jnp.zeros((ROWS, LANES), jnp.float32)
        for X in range(xc):
            v = jnp.where(low_half, coarse[level, g, 2 + X, 0], coarse[level, g, 2 + X, tiles - 1])
            packed = jnp.where(lane // 8 == X, roll(v, 8 * X + 4, 1), packed)
        czs[w, g] = packed
        start(coarse_copies(level, w, g))

    def z_edges(w, i, g):
        if nz > 2:
            return jnp.where(first_of_eight, czr[w, i, 0, g], czr[w, i, 1, g])
        return czr[w, i, 0, g]

    def z_halo(packed, X):
        return roll(packed, -(8 * X + 4), 1)

    def update(v, s, rhs):
        return (1.0 - WEIGHT) * v + (0.125 * WEIGHT / COARSE_DIAG) * s + rhs

    def sweep_plane(zero, level, g, X, hz):
        vs = [coarse[level, g, 2 + X, t] for t in range(tiles)]
        z = shifted_z(vs, hz, 2)
        for t in range(tiles):
            s = coarse[level, g, 1 + X, t] + coarse[level, g, 3 + X, t]
            s = s + shifted_y(vs[t], beside[level, g, 1 + X, t], 2) + z[t]
            coarse[level + 1, g, 2 + X, t] = update(vs[t], s, coarse[zero, g, 2 + X, t])

    def sweep_wide(zero, level, w, g):
        zc, from_left, from_right, zy = (z_edges(w, i, g) for i in range(4))
        zs = czs[w, g]
        for X in range(-1, xc + 1):
            if X < 0:
                hz = z_halo(from_left, xc - 1)
            elif X == xc:
                hz = z_halo(from_right, 0)
            else:
                hz = z_halo(zc, X)
            sweep_plane(zero, level, g, X, hz)
        for X in range(xc):
            hs = [beside[level, g, 1 + X, t] for t in range(tiles)]
            z = shifted_z(hs, z_halo(zy, X), 2)
            for t in range(tiles):
                h, v = hs[t], coarse[level, g, 2 + X, t]
                y = jnp.where(top_half, roll(h, -2, 0) + roll(v, 2, 0), roll(h, 2, 0) + roll(v, -2, 0))
                s = beside[level, g, X, t] + beside[level, g, 2 + X, t] + y + z[t]
                beside[level + 1, g, 1 + X, t] = update(h, s, beside[zero, g, 1 + X, t])
        edge = 8 * (xc - 1)
        s = jnp.where(lane < 8, roll(from_left, -edge, 1), roll(zc, 8, 1))
        s = s + jnp.where(lane >= edge, roll(from_right, edge, 1), roll(zc, -8, 1))
        s = s + shifted_y(zc, zy, 2)
        s = s + jnp.where(
            first_of_eight, roll(zc, 2, 1) + roll(zs, -2, 1), roll(zc, -2, 1) + roll(zs, 2, 1)
        )
        czm[w, g] = update(zc, s, z_edges(w // 2 * 2, 0, g))

    def sweep_own(zero, level, w, g):
        zc = czm[w, g]
        for X in range(xc):
            sweep_plane(zero, level, g, X, z_halo(zc, X))

    def spread(p):
        out = []
        for v in (jnp.where(even_row, p, roll(p, 1, 0)), jnp.where(even_row, roll(p, -1, 0), p)):
            out.append(jnp.where(even_lane, v, roll(v, 1, 1)))
            out.append(jnp.where(even_lane, roll(v, -1, 1), v))
        return out

    def prolong(level, w, g, use):
        zc = czm[w, g]
        for X in range(xc + 2):
            for t in range(tiles):
                for k, v in enumerate(spread(coarse[level, g, 1 + X, t])):
                    dup[k, X, t] = v
        for X in range(xc):
            for t in range(tiles):
                for k, v in enumerate(spread(beside[level, g, 1 + X, t])):
                    duph[k, X, t] = v
            for k, v in enumerate(spread(z_halo(zc, X))):
                dupz[k, X] = v

        def one(b):
            k = lax.rem(b, QUAD)
            for X in range(xc):
                vs = [dup[k, 1 + X, t] for t in range(tiles)]
                z = shifted_z(vs, dupz[k, X], 1)
                for t in range(tiles):
                    s = shifted_y(vs[t], duph[k, X, t], 1) + z[t] + vs[t]
                    for x, other in ((2 * X, X), (2 * X + 1, 2 + X)):
                        total = s + dup[k, other, t]
                        kr = (1.0 - WEIGHT) * (res[b, 2 + x, t] + vs[t] + rem[b, x, t]) + (
                            0.5 * WEIGHT / 4.0
                        ) * total
                        use(b, x, t, kr)

        loop(g * per, (g + 1) * per, one)

    def apply_one(g, b):
        norm, energy = [], []

        def use(x, vs, outs):
            for t in range(tiles):
                app[b, 2 + x, t] = outs[t]
                norm.append(vs[t] * vs[t])
                energy.append(vs[t] * outs[t])

        hamiltonian(orb, 0, b, use)
        acc[0, g, pl.ds(b - g * per, 1), :] = rowsum(norm)
        acc[0, g, pl.ds(b - g * per + per, 1), :] = rowsum(energy)

    def prepare_first(b):
        e = get(0, b)
        for x in range(1, xs + 3):
            for t in range(tiles):
                res[b, x, t] = app[b, x, t] - e * orb[b, x, t]

        def ry(s, j, t):
            return fyr[1][s, b, 0, t] - e * fyr[0][s, b, 1 - s, t]

        restrict(b, ry, z_packed(fzr[1], b) - e * z_packed(fzr[0], b))

    def use_first(b, x, t, kr):
        cor[b, 2 + x, t] = kr

    def respond_one(g, b):
        e = get(0, b)
        dots = [None] * NDOTS

        def use(x, vs, outs):
            for t in range(tiles):
                c, o, r = vs[t], orb[b, 2 + x, t], res[b, 2 + x, t]
                p = outs[t] - e * c
                rsp[b, 2 + x, t] = p
                for q, (u, v) in enumerate(((r, p), (p, p), (o, c), (c, c), (p, o), (p, c), (r, o), (r, c))):
                    w = u * v
                    dots[q] = w if dots[q] is None else dots[q] + w

        hamiltonian(cor, 2, b, use)
        for q in range(NDOTS):
            acc[1, g, pl.ds(b - g * per + q * per, 1), :] = rowsum([dots[q]])

    def prepare_second(b):
        e, ml, mc, mcl = get(0, b), get(2, b), get(3, b), get(4, b)

        def mixed(r, p, o, c):
            return r + ml * p - mc * o - mcl * c

        for x in range(1, xs + 3):
            for t in range(tiles):
                res[b, x, t] = mixed(res[b, x, t], rsp[b, x, t], orb[b, x, t], cor[b, x, t])

        def ry(s, j, t):
            o = fyr[0][s, b, 1 - s, t]
            r = fyr[1][s, b, 0, t] - e * o
            return mixed(r, fyr[3][s, b, 0, t], o, fyr[2][s, b, 1 - s, t])

        oz = z_packed(fzr[0], b)
        rz = z_packed(fzr[1], b) - e * oz
        restrict(b, ry, mixed(rz, z_packed(fzr[3], b), oz, z_packed(fzr[2], b)))

    def use_second(b, x, t, kr):
        out[b, x, :, t * LANES : (t + 1) * LANES] = (
            orb[b, 2 + x, t] + get(2, b) * cor[b, 2 + x, t] + get(1, b) * kr
        )

    def coarse_begin(turn, g):
        coarse_pack(turn * COARSE_SWEEPS, g)
        coarse_send(turn * COARSE_SWEEPS, 2 * turn, g)

    def coarse_solve(turn, use, then):
        zero = turn * COARSE_SWEEPS
        w = 2 * turn

        def middle(g):
            wait(coarse_copies(zero, w, g))
            sweep_wide(zero, zero, w, g)
            sweep_own(zero, zero + 1, w, g)
            coarse_send(zero + 2, w + 1, g)

        def finish(g):
            wait(coarse_copies(zero + 2, w + 1, g))
            sweep_wide(zero, zero + 2, w + 1, g)
            prolong(zero + 3, w + 1, g, use)
            then(g)

        loop(0, GROUPS, middle)
        loop(0, GROUPS, finish)

    def begin(g):
        wait(load_copies(g))
        fine_send(orb, 0, 2, g)

    def first_hamiltonian(g):
        wait(fine_copies(orb, 0, 2, g))
        loop(g * per, (g + 1) * per, functools.partial(apply_one, g))
        reduce_start(0, g, 2)
        fine_send(app, 1, 1, g)

    def first_residual(g):
        norm_orbitals, first_energy = reduce_finish(0, g, 2)
        energy = first_energy / (norm_orbitals + EPSILON)
        for i, v in enumerate((norm_orbitals, first_energy, energy)):
            keep[i, g] = v
        put(0, g, energy)
        wait(fine_copies(app, 1, 1, g))
        loop(g * per, (g + 1) * per, prepare_first)
        coarse_begin(0, g)

    def second_hamiltonian(g):
        wait(fine_copies(cor, 2, 2, g))
        loop(g * per, (g + 1) * per, functools.partial(respond_one, g))
        reduce_start(1, g, NDOTS)
        fine_send(rsp, 3, 1, g)

    def second_residual(g):
        norm_orbitals, first_energy, energy = (keep[i, g] for i in range(3))
        rp, pp, oc, cc, po, pc, ro, rc = reduce_finish(1, g, NDOTS)
        lam = -rp / (pp + EPSILON)
        trial_norm = norm_orbitals + 2.0 * lam * oc + lam * lam * cc
        trial_sum = (
            first_energy + lam * ((po + energy * oc) + (rc + energy * oc)) + lam * lam * (pc + energy * cc)
        )
        trial = trial_sum / (trial_norm + EPSILON)
        energies[pl.ds(g, 1), :] = trial[0:1]
        change = trial - energy
        projected = lam * rp - change * (ro + lam * rc)
        cross = po + lam * pc
        change_norm = lam * lam * pp - 2.0 * lam * change * cross + change * change * trial_norm
        mix = -projected / (change_norm + EPSILON)
        put(1, g, lam)
        put(2, g, mix * lam)
        put(3, g, mix * change)
        put(4, g, mix * change * lam)
        wait(fine_copies(rsp, 3, 1, g))
        loop(g * per, (g + 1) * per, prepare_second)
        coarse_begin(1, g)

    greeted(barrier, (0, 1, 2))
    greet(greet_y, (1,))
    loop(0, GROUPS, begin)
    greeted(greet_y, (1,))
    greet(greet_z, (2,))
    pot_load.wait()
    greeted(greet_z, (2,))
    loop(0, GROUPS, first_hamiltonian)
    loop(0, GROUPS, first_residual)
    coarse_solve(0, use_first, lambda g: fine_send(cor, 2, 2, g))
    loop(0, GROUPS, second_hamiltonian)
    loop(0, GROUPS, second_residual)
    coarse_solve(1, use_second, lambda g: None)


def solution(mesh):
    sizes = tuple(mesh.shape[a] for a in AXES)

    def body(orbitals, potential):
        bands, xs, ys, zs = orbitals.shape
        tiles = zs // LANES
        tile = (ROWS, LANES)
        vmem = lambda *s: pltpu.VMEM(s + tile, jnp.float32)
        field = vmem(bands, xs + 4, tiles)
        moves = 8 + 5 * (1 if sizes[2] == 2 else 2)
        assert bands == QUAD * GROUPS
        devices = sizes[0] * sizes[1] * sizes[2]
        per = bands // GROUPS

        def call(*refs):
            refs = list(refs)
            head, rest = refs[:4], refs[4:]
            fields, rest = rest[:7], rest[7:]
            fys, rest = rest[:4], rest[4:]
            fyr, rest = rest[:4], rest[4:]
            fzs, rest = rest[:4], rest[4:]
            fzr, rest = rest[:4], rest[4:]
            kernel(sizes, *head, *fields, fys, fyr, fzs, fzr, *rest)

        depths = (2, 1, 2, 1)
        updated, trial = pl.pallas_call(
            call,
            out_shape=(
                jax.ShapeDtypeStruct(orbitals.shape, jnp.float32),
                jax.ShapeDtypeStruct(tile, jnp.float32),
            ),
            in_specs=[
                pl.BlockSpec(memory_space=pltpu.HBM),
                pl.BlockSpec(memory_space=pltpu.HBM),
            ],
            out_specs=(
                pl.BlockSpec(memory_space=pltpu.VMEM),
                pl.BlockSpec(memory_space=pltpu.VMEM),
            ),
            scratch_shapes=[field] * 5
            + [vmem(bands, xs, tiles), vmem(2 * COARSE_SWEEPS, GROUPS, xs // 2 + 4, tiles)]
            + [vmem(2, bands, d, tiles) for d in depths]
            + [vmem(2, bands, d, tiles) for d in depths]
            + [vmem(bands) for d in depths]
            + [vmem(2, bands) for d in depths]
            + [
                vmem(bands, xs, tiles),
                vmem(2 * COARSE_SWEEPS, GROUPS, xs // 2 + 2, tiles),
                vmem(4, GROUPS),
                vmem(4, 4, 2, GROUPS),
                vmem(4, GROUPS),
                vmem(QUAD, xs // 2 + 2, tiles),
                vmem(QUAD, xs // 2, tiles),
                vmem(QUAD, xs // 2),
                pltpu.VMEM((2, GROUPS, NDOTS * per, LANES), jnp.float32),
                pltpu.VMEM((5, bands, LANES), jnp.float32),
                vmem(3, GROUPS),
                pltpu.VMEM((2 * GROUPS, devices, 1, LANES), jnp.float32),
                pltpu.VMEM(potential.shape, jnp.float32),
                pltpu.SemaphoreType.DMA((GROUPS + 1, tiles)),
                pltpu.SemaphoreType.DMA((GROUPS, moves)),
                pltpu.SemaphoreType.DMA((2, GROUPS, moves)),
                pltpu.SemaphoreType.DMA((2 * GROUPS,)),
                pltpu.SemaphoreType.DMA((2 * GROUPS,)),
                pltpu.SemaphoreType.REGULAR,
                pltpu.SemaphoreType.REGULAR,
            ],
            compiler_params=pltpu.CompilerParams(
                collective_id=0, has_side_effects=True, vmem_limit_bytes=53760 * 1024
            ),
        )(orbitals, potential)
        return updated, trial[:GROUPS, :per].reshape(bands)

    return jax.shard_map(
        body,
        mesh=mesh,
        in_specs=(P(None, "gx", "gy", "gz"), P("gx", "gy", "gz")),
        out_specs=(P(None, "gx", "gy", "gz"), P()),
        check_vma=False,
    )
```

```python
import functools
import math

import jax
import jax.numpy as jnp
from jax import lax
from jax.experimental import pallas as pl
from jax.experimental.pallas import tpu as pltpu
from jax.sharding import PartitionSpec as P

COARSE_SWEEPS = 4
QUAD = 4
AHEAD = 2
WEIGHT = 0.8
COARSE_DIAG = 1.75
EPSILON = 1e-06
LANES = 128
ROWS = 8
GROUPS = 4
AXES = ("gx", "gy", "gz")
MESH = pl.DeviceIdType.MESH
NDOTS = 8


def kernel(sizes, orb_hbm, pot_hbm, out, energies, *scratch):
    (
        orb, app, res, cor, rsp, rem, coarse,
        fys, fyr, fzs, fzr, hy, beside, czs, czr, czm, dup, duph, dupz,
        acc, scal, keep, red, pot, blank, load_sem, send_sem, recv_sem, rsend, rrecv, greet_y, greet_z,
    ) = scratch
    nx, ny, nz = sizes
    bands, xs = orb_hbm.shape[0], orb_hbm.shape[1]
    tiles = orb_hbm.shape[3] // LANES
    xc = xs // 2
    per = bands // GROUPS
    devices = nx * ny * nz
    me = [lax.axis_index(a) for a in AXES]
    right = [lax.rem(m + 1, n) for m, n in zip(me, sizes)]
    left = [lax.rem(m + n - 1, n) for m, n in zip(me, sizes)]

    here = (me[0] * ny + me[1]) * nz + me[2]

    def start(copies):
        for c in copies:
            c.start()

    def wait(copies):
        for c in copies:
            c.wait()

    pot_load = pltpu.make_async_copy(pot_hbm, pot, load_sem.at[GROUPS, 0])

    def load_copies(g):
        part = pl.ds(g * per, per)
        return [
            pltpu.make_async_copy(
                orb_hbm.at[part, :, :, pl.ds(t * LANES, LANES)],
                orb.at[part, pl.ds(2, xs), t],
                load_sem.at[g, t],
            )
            for t in range(tiles)
        ]

    for g in range(GROUPS):
        start(load_copies(g))
    pot_load.start()

    def wrap(k, d):
        return lax.rem(me[k] + d, sizes[k])

    def every_peer(f):
        if devices <= 64:
            xyz = [[me[k]] + [wrap(k, d) for d in range(1, sizes[k])] for k in range(3)]
            for d in range(1, devices):
                f((xyz[0][d // (ny * nz)], xyz[1][d // nz % ny], xyz[2][d % nz]))
        else:

            def step(d, carry):
                f((wrap(0, d // (ny * nz)), wrap(1, lax.rem(d // nz, ny)), wrap(2, lax.rem(d, nz))))
                return carry

            lax.fori_loop(1, devices, step, 0)

    for level in (0, 2):
        for turn in range(2):
            for X in (0, 1 + xc):
                for g in range(GROUPS):
                    for t in range(tiles):
                        beside[turn * COARSE_SWEEPS + level, g, X, t] = jnp.zeros((ROWS, LANES), jnp.float32)

    def greet(semaphore, axes):
        for k in axes:
            for d in range(1, sizes[k]):
                pl.semaphore_signal(semaphore, inc=1, device_id={AXES[k]: wrap(k, d)}, device_id_type=MESH)

    def greeted(semaphore, axes):
        pl.semaphore_wait(semaphore, sum(sizes[k] - 1 for k in axes))

    barrier = pltpu.get_barrier_semaphore()
    greet(barrier, (0, 1, 2))

    row = lax.broadcasted_iota(jnp.int32, (ROWS, LANES), 0)
    lane = lax.broadcasted_iota(jnp.int32, (ROWS, LANES), 1)
    even_lane = lane % 2 == 0
    even_row = row % 2 == 0
    low_half = lane < LANES // 2
    first_of_four = lane % 4 < 2
    first_of_eight = lane % 8 < 4
    top_half = row < ROWS // 2

    z_ends = (right[2], left[2])[: 1 if nz == 2 else 2]

    def roll(v, k, axis):
        return pltpu.roll(v, k % v.shape[axis], axis)

    def flat(ref):
        n = 1
        for s in ref.shape[:-1]:
            n *= s
        return ref.reshape(n, LANES)

    def loop(lo, hi, f):
        def step(i, carry):
            f(i)
            return carry

        lax.fori_loop(lo, hi, step, 0)

    def send(moves, turn, g):
        for src, dst, to in moves:
            pltpu.make_async_remote_copy(
                src_ref=src,
                dst_ref=dst,
                send_sem=send_sem.at[g],
                recv_sem=recv_sem.at[turn % 2, g],
                device_id=to,
                device_id_type=MESH,
            ).start()

    def arrive(moves, turn, g):
        part = blank.at[pl.ds(0, sum(math.prod(src.shape) for src, _, _ in moves) // LANES)]
        pltpu.make_async_copy(part, part, recv_sem.at[turn % 2, g]).wait()
        pltpu.make_async_copy(part, part, send_sem.at[g]).wait()

    def fine_moves(field, which, depth, g):
        part = pl.ds(g * per, per)
        ys, yr = fys[which], fyr[which]
        zs, zr = fzs[which], fzr[which]
        moves = [
            (field.at[part, pl.ds(2 + xs - depth, depth)], field.at[part, pl.ds(2 - depth, depth)], {"gx": right[0]}),
            (field.at[part, pl.ds(2, depth)], field.at[part, pl.ds(2 + xs, depth)], {"gx": left[0]}),
            (ys.at[0, part], yr.at[0, part], {"gy": right[1]}),
            (ys.at[1, part], yr.at[1, part], {"gy": left[1]}),
        ]
        for end, z in enumerate(z_ends):
            moves.append((zs.at[part], zr.at[end, part], {"gz": z}))
        return moves

    def fine_pack(field, which, depth, g):
        view = flat(field)
        span = field.shape[1]
        ys, zs = fys[which], fzs[which]

        def pack(b):
            for t in range(tiles):
                for j in range(depth):
                    base = ((b * span + 2) * tiles + t) * ROWS
                    ys[0, b, j, t] = view[pl.ds(base + ROWS - depth + j, xs, stride=tiles * ROWS), :]
                    ys[1, b, j, t] = view[pl.ds(base + j, xs, stride=tiles * ROWS), :]
            packed = jnp.zeros((ROWS, LANES), jnp.float32)
            for x in range(xs):
                w = jnp.where(low_half, field[b, 2 + x, 0], field[b, 2 + x, tiles - 1])
                packed = jnp.where(lane // 4 == x, roll(w, 2 + 4 * x, 1), packed)
            zs[b] = packed

        for k in range(per):
            pack(g * per + k)

    def fine_send(field, which, depth, g):
        fine_pack(field, which, depth, g)
        send(fine_moves(field, which, depth, g), which, g)

    def fine_arrive(field, which, depth, g):
        arrive(fine_moves(field, which, depth, g), which, g)

    def z_packed(zr, b):
        if nz > 2:
            return jnp.where(first_of_four, zr[0, b], zr[1, b])
        return zr[0, b]

    def unpack_y(yr, b, depth):
        view = flat(hy)
        for t in range(tiles):
            for j in range(depth):
                base = (b * xs * tiles + t) * ROWS
                view[pl.ds(base + ROWS - depth + j, xs, stride=tiles * ROWS), :] = yr(0, j, t)
                view[pl.ds(base + j, xs, stride=tiles * ROWS), :] = yr(1, j, t)

    def shifted_y(v, h, k):
        up = roll(jnp.where(row >= ROWS - k, h, v), k, 0)
        down = roll(jnp.where(row < k, h, v), -k, 0)
        return up + down

    def shifted_z(vs, hz, k):
        before = [hz] + vs[:-1]
        after = vs[1:] + [hz]
        return [
            roll(jnp.where(lane >= LANES - k, p, v), k, 1) + roll(jnp.where(lane < k, n, v), -k, 1)
            for p, v, n in zip(before, vs, after)
        ]

    def hamiltonian(field, which, b, use):
        unpack_y(lambda s, j, t: fyr[which][s, b, j, t], b, 2)
        zp = z_packed(fzr[which], b)
        for x in range(xs):
            hz = roll(zp, -(4 * x + 2), 1)
            vs = [field[b, 2 + x, t] for t in range(tiles)]
            z1, z2 = shifted_z(vs, hz, 1), shifted_z(vs, hz, 2)
            outs = []
            for t in range(tiles):
                h = hy[b, x, t]
                near = field[b, 1 + x, t] + field[b, 3 + x, t] + shifted_y(vs[t], h, 1) + z1[t]
                far = field[b, x, t] + field[b, 4 + x, t] + shifted_y(vs[t], h, 2) + z2[t]
                potential = pot[x, :, t * LANES : (t + 1) * LANES]
                outs.append((potential + 3.75) * vs[t] - (2.0 / 3.0) * near + (1.0 / 24.0) * far)
            use(x, vs, outs)

    def rowsum(vs):
        return jnp.sum(functools.reduce(jnp.add, vs), axis=0, keepdims=True)

    def reduce_start(index, g, ndots):
        total = jnp.zeros((ROWS, LANES), jnp.float32)
        for i in range(ndots * per // ROWS):
            part = jnp.sum(acc[index, g, i * ROWS : (i + 1) * ROWS, :], axis=1, keepdims=True)
            total = jnp.where(lane == row + i * ROWS, part, total)
        k = index * GROUPS + g
        red[k, here] = jnp.sum(total, axis=0, keepdims=True)

        def send(to):
            pltpu.make_async_remote_copy(
                src_ref=red.at[k, here],
                dst_ref=red.at[k, here],
                send_sem=rsend.at[k],
                recv_sem=rrecv.at[k],
                device_id=to,
                device_id_type=MESH,
            ).start()

        every_peer(send)

    def reduce_finish(index, g, ndots):
        k = index * GROUPS + g
        rest = red.at[k, pl.ds(0, devices - 1)]
        pltpu.make_async_copy(rest, rest, rrecv.at[k]).wait()
        pltpu.make_async_copy(rest, rest, rsend.at[k]).wait()
        total = jnp.broadcast_to(jnp.sum(red[k], axis=0), (ROWS, LANES))
        return [total if q == 0 else roll(total, -q * per, 1) for q in range(ndots)]

    def put(k, g, values):
        for b in range(per):
            scal[k, pl.ds(g * per + b, 1), :] = jnp.broadcast_to(values[0:1, b : b + 1], (1, LANES))

    def get(k, b):
        return scal[k, pl.ds(b, 1), :]

    def restrict(b, ry, rz):
        k = lax.rem(b, QUAD)
        unpack_y(ry, b, 1)
        for X in range(xc):
            pair = [None] * tiles
            for x in (2 * X, 2 * X + 1):
                hz = roll(rz, -(4 * x + 2), 1)
                vs = [res[b, 2 + x, t] for t in range(tiles)]
                z1 = shifted_z(vs, hz, 1)
                for t in range(tiles):
                    s = res[b, 1 + x, t] + res[b, 3 + x, t] + shifted_y(vs[t], hy[b, x, t], 1) + z1[t]
                    m = (1.0 - WEIGHT) * vs[t] + (0.5 * WEIGHT / 4.0) * s
                    rem[b, x, t] = m
                    pair[t] = m if pair[t] is None else pair[t] + m
            for t in range(tiles):
                s = pair[t]
                s = s + jnp.where(even_row, roll(s, -1, 0), roll(s, 1, 0))
                s = s + jnp.where(even_lane, roll(s, -1, 1), roll(s, 1, 1))
                dup[k, 1 + X, t] = s * (0.125 * WEIGHT / COARSE_DIAG)

    def coarse_pack(level, g):
        for X in range(xc):
            for t in range(tiles):
                lanes = [jnp.where(even_lane, dup[k, 1 + X, t], dup[k + 1, 1 + X, t]) for k in (0, 2)]
                coarse[level, g, 2 + X, t] = jnp.where(even_row, lanes[0], lanes[1])

    def coarse_moves(level, w, g):
        own, side = coarse.at[level, g], beside.at[level, g]
        low, high = pl.ds(0, ROWS // 2), pl.ds(ROWS // 2, ROWS // 2)
        top, bottom = pl.ds(0, 2), pl.ds(ROWS - 2, 2)
        inner, last, first = pl.ds(2, xc), 1 + xc, 2
        right_x, left_x = {"gx": right[0]}, {"gx": left[0]}
        right_y, left_y = {"gy": right[1]}, {"gy": left[1]}
        moves = [
            (own.at[pl.ds(xc, 2)], own.at[pl.ds(0, 2)], right_x),
            (own.at[pl.ds(2, 2)], own.at[pl.ds(2 + xc, 2)], left_x),
            (own.at[inner, :, high], side.at[pl.ds(1, xc), :, high], right_y),
            (own.at[inner, :, low], side.at[pl.ds(1, xc), :, low], left_y),
        ]
        for end, z in enumerate(z_ends):
            moves.append((czs.at[w, g], czr.at[w, 0, end, g], {"gz": z}))
        moves += [
            (own.at[last, :, bottom], side.at[0, :, bottom], right_x | right_y),
            (own.at[last, :, top], side.at[0, :, top], right_x | left_y),
            (own.at[first, :, bottom], side.at[1 + xc, :, bottom], left_x | right_y),
            (own.at[first, :, top], side.at[1 + xc, :, top], left_x | left_y),
        ]
        for end, z in enumerate(z_ends):
            for i, to in ((1, right_x), (2, left_x)):
                moves.append((czs.at[w, g], czr.at[w, i, end, g], to | {"gz": z}))
            for part, to in ((bottom, right_y), (top, left_y)):
                moves.append((czs.at[w, g, part], czr.at[w, 3, end, g, part], to | {"gz": z}))
        return moves

    def coarse_send(level, w, g):
        packed = jnp.zeros((ROWS, LANES), jnp.float32)
        for X in range(xc):
            v = jnp.where(low_half, coarse[level, g, 2 + X, 0], coarse[level, g, 2 + X, tiles - 1])
            packed = jnp.where(lane // 8 == X, roll(v, 8 * X + 4, 1), packed)
        czs[w, g] = packed
        send(coarse_moves(level, w, g), w, g)

    def z_edges(w, i, g):
        if nz > 2:
            return jnp.where(first_of_eight, czr[w, i, 0, g], czr[w, i, 1, g])
        return czr[w, i, 0, g]

    def z_halo(packed, X):
        return roll(packed, -(8 * X + 4), 1)

    def update(v, s, rhs):
        return (1.0 - WEIGHT) * v + (0.125 * WEIGHT / COARSE_DIAG) * s + rhs

    def sweep_plane(zero, level, g, X, hz):
        vs = [coarse[level, g, 2 + X, t] for t in range(tiles)]
        z = shifted_z(vs, hz, 2)
        for t in range(tiles):
            s = coarse[level, g, 1 + X, t] + coarse[level, g, 3 + X, t]
            s = s + shifted_y(vs[t], beside[level, g, 1 + X, t], 2) + z[t]
            coarse[level + 1, g, 2 + X, t] = update(vs[t], s, coarse[zero, g, 2 + X, t])

    def sweep_wide(zero, level, w, g):
        zc, from_left, from_right, zy = (z_edges(w, i, g) for i in range(4))
        zs = czs[w, g]
        for X in range(-1, xc + 1):
            if X < 0:
                hz = z_halo(from_left, xc - 1)
            elif X == xc:
                hz = z_halo(from_right, 0)
            else:
                hz = z_halo(zc, X)
            sweep_plane(zero, level, g, X, hz)
        for X in range(xc):
            hs = [beside[level, g, 1 + X, t] for t in range(tiles)]
            z = shifted_z(hs, z_halo(zy, X), 2)
            for t in range(tiles):
                h, v = hs[t], coarse[level, g, 2 + X, t]
                y = jnp.where(top_half, roll(h, -2, 0) + roll(v, 2, 0), roll(h, 2, 0) + roll(v, -2, 0))
                s = beside[level, g, X, t] + beside[level, g, 2 + X, t] + y + z[t]
                beside[level + 1, g, 1 + X, t] = update(h, s, beside[zero, g, 1 + X, t])
        edge = 8 * (xc - 1)
        s = jnp.where(lane < 8, roll(from_left, -edge, 1), roll(zc, 8, 1))
        s = s + jnp.where(lane >= edge, roll(from_right, edge, 1), roll(zc, -8, 1))
        s = s + shifted_y(zc, zy, 2)
        s = s + jnp.where(
            first_of_eight, roll(zc, 2, 1) + roll(zs, -2, 1), roll(zc, -2, 1) + roll(zs, 2, 1)
        )
        czm[w, g] = update(zc, s, z_edges(w // 2 * 2, 0, g))

    def sweep_own(zero, level, w, g):
        zc = czm[w, g]
        for X in range(xc):
            sweep_plane(zero, level, g, X, z_halo(zc, X))

    def spread(p):
        out = []
        for v in (jnp.where(even_row, p, roll(p, 1, 0)), jnp.where(even_row, roll(p, -1, 0), p)):
            out.append(jnp.where(even_lane, v, roll(v, 1, 1)))
            out.append(jnp.where(even_lane, roll(v, -1, 1), v))
        return out

    def prolong(level, w, g, use):
        zc = czm[w, g]
        for X in range(xc + 2):
            for t in range(tiles):
                for k, v in enumerate(spread(coarse[level, g, 1 + X, t])):
                    dup[k, X, t] = v
        for X in range(xc):
            for t in range(tiles):
                for k, v in enumerate(spread(beside[level, g, 1 + X, t])):
                    duph[k, X, t] = v
            for k, v in enumerate(spread(z_halo(zc, X))):
                dupz[k, X] = v

        def one(b):
            k = lax.rem(b, QUAD)
            for X in range(xc):
                vs = [dup[k, 1 + X, t] for t in range(tiles)]
                z = shifted_z(vs, dupz[k, X], 1)
                for t in range(tiles):
                    s = shifted_y(vs[t], duph[k, X, t], 1) + z[t] + vs[t]
                    for x, other in ((2 * X, X), (2 * X + 1, 2 + X)):
                        total = s + dup[k, other, t]
                        kr = (1.0 - WEIGHT) * (res[b, 2 + x, t] + vs[t] + rem[b, x, t]) + (
                            0.5 * WEIGHT / 4.0
                        ) * total
                        use(b, x, t, kr)

        loop(g * per, (g + 1) * per, one)

    def apply_one(g, b):
        norm, energy = [], []

        def use(x, vs, outs):
            for t in range(tiles):
                app[b, 2 + x, t] = outs[t]
                norm.append(vs[t] * vs[t])
                energy.append(vs[t] * outs[t])

        hamiltonian(orb, 0, b, use)
        acc[0, g, pl.ds(b - g * per, 1), :] = rowsum(norm)
        acc[0, g, pl.ds(b - g * per + per, 1), :] = rowsum(energy)

    def prepare_first(b):
        e = get(0, b)
        for x in range(1, xs + 3):
            for t in range(tiles):
                res[b, x, t] = app[b, x, t] - e * orb[b, x, t]

        def ry(s, j, t):
            return fyr[1][s, b, 0, t] - e * fyr[0][s, b, 1 - s, t]

        restrict(b, ry, z_packed(fzr[1], b) - e * z_packed(fzr[0], b))

    def use_first(b, x, t, kr):
        cor[b, 2 + x, t] = kr

    def respond_one(g, b):
        e = get(0, b)
        dots = [None] * NDOTS

        def use(x, vs, outs):
            for t in range(tiles):
                c, o, r = vs[t], orb[b, 2 + x, t], res[b, 2 + x, t]
                p = outs[t] - e * c
                rsp[b, 2 + x, t] = p
                for q, (u, v) in enumerate(((r, p), (p, p), (o, c), (c, c), (p, o), (p, c), (r, o), (r, c))):
                    w = u * v
                    dots[q] = w if dots[q] is None else dots[q] + w

        hamiltonian(cor, 2, b, use)
        for q in range(NDOTS):
            acc[1, g, pl.ds(b - g * per + q * per, 1), :] = rowsum([dots[q]])

    def prepare_second(b):
        e, ml, mc, mcl = get(0, b), get(2, b), get(3, b), get(4, b)

        def mixed(r, p, o, c):
            return r + ml * p - mc * o - mcl * c

        for x in range(1, xs + 3):
            for t in range(tiles):
                res[b, x, t] = mixed(res[b, x, t], rsp[b, x, t], orb[b, x, t], cor[b, x, t])

        def ry(s, j, t):
            o = fyr[0][s, b, 1 - s, t]
            r = fyr[1][s, b, 0, t] - e * o
            return mixed(r, fyr[3][s, b, 0, t], o, fyr[2][s, b, 1 - s, t])

        oz = z_packed(fzr[0], b)
        rz = z_packed(fzr[1], b) - e * oz
        restrict(b, ry, mixed(rz, z_packed(fzr[3], b), oz, z_packed(fzr[2], b)))

    def use_second(b, x, t, kr):
        out[b, x, :, t * LANES : (t + 1) * LANES] = (
            orb[b, 2 + x, t] + get(2, b) * cor[b, 2 + x, t] + get(1, b) * kr
        )

    def coarse_begin(turn, g):
        coarse_pack(turn * COARSE_SWEEPS, g)
        coarse_send(turn * COARSE_SWEEPS, 2 * turn, g)

    def coarse_solve(turn, use, then):
        zero = turn * COARSE_SWEEPS
        w = 2 * turn

        def middle(g):
            arrive(coarse_moves(zero, w, g), w, g)
            sweep_wide(zero, zero, w, g)
            sweep_own(zero, zero + 1, w, g)
            coarse_send(zero + 2, w + 1, g)

        def finish(g):
            arrive(coarse_moves(zero + 2, w + 1, g), w + 1, g)
            sweep_wide(zero, zero + 2, w + 1, g)
            prolong(zero + 3, w + 1, g, use)
            then(g)

        loop(0, GROUPS, middle)
        loop(0, GROUPS, finish)

    def begin(g):
        wait(load_copies(g))
        fine_send(orb, 0, 2, g)

    def first_hamiltonian(g):
        fine_arrive(orb, 0, 2, g)
        loop(g * per, (g + 1) * per, functools.partial(apply_one, g))
        reduce_start(0, g, 2)
        fine_send(app, 1, 1, g)

    def first_residual(g):
        norm_orbitals, first_energy = reduce_finish(0, g, 2)
        energy = first_energy / (norm_orbitals + EPSILON)
        for i, v in enumerate((norm_orbitals, first_energy, energy)):
            keep[i, g] = v
        put(0, g, energy)
        fine_arrive(app, 1, 1, g)
        loop(g * per, (g + 1) * per, prepare_first)
        coarse_begin(0, g)

    def second_hamiltonian(g):
        fine_arrive(cor, 2, 2, g)
        loop(g * per, (g + 1) * per, functools.partial(respond_one, g))
        reduce_start(1, g, NDOTS)
        fine_send(rsp, 3, 1, g)

    def second_residual(g):
        norm_orbitals, first_energy, energy = (keep[i, g] for i in range(3))
        rp, pp, oc, cc, po, pc, ro, rc = reduce_finish(1, g, NDOTS)
        lam = -rp / (pp + EPSILON)
        trial_norm = norm_orbitals + 2.0 * lam * oc + lam * lam * cc
        trial_sum = (
            first_energy + lam * ((po + energy * oc) + (rc + energy * oc)) + lam * lam * (pc + energy * cc)
        )
        trial = trial_sum / (trial_norm + EPSILON)
        energies[pl.ds(g, 1), :] = trial[0:1]
        change = trial - energy
        projected = lam * rp - change * (ro + lam * rc)
        cross = po + lam * pc
        change_norm = lam * lam * pp - 2.0 * lam * change * cross + change * change * trial_norm
        mix = -projected / (change_norm + EPSILON)
        put(1, g, lam)
        put(2, g, mix * lam)
        put(3, g, mix * change)
        put(4, g, mix * change * lam)
        fine_arrive(rsp, 3, 1, g)
        loop(g * per, (g + 1) * per, prepare_second)
        coarse_begin(1, g)

    for g in range(AHEAD):
        wait(load_copies(g))
        fine_pack(orb, 0, 2, g)
    greeted(barrier, (0, 1, 2))
    for g in range(AHEAD):
        send(fine_moves(orb, 0, 2, g), 0, g)
    greet(greet_y, (1,))
    loop(AHEAD, GROUPS, begin)
    greeted(greet_y, (1,))
    greet(greet_z, (2,))
    pot_load.wait()
    greeted(greet_z, (2,))
    loop(0, GROUPS, first_hamiltonian)
    loop(0, GROUPS, first_residual)
    coarse_solve(0, use_first, lambda g: fine_send(cor, 2, 2, g))
    loop(0, GROUPS, second_hamiltonian)
    loop(0, GROUPS, second_residual)
    coarse_solve(1, use_second, lambda g: None)


def solution(mesh):
    sizes = tuple(mesh.shape[a] for a in AXES)

    def body(orbitals, potential):
        bands, xs, ys, zs = orbitals.shape
        tiles = zs // LANES
        tile = (ROWS, LANES)
        vmem = lambda *s: pltpu.VMEM(s + tile, jnp.float32)
        field = vmem(bands, xs + 4, tiles)
        assert bands == QUAD * GROUPS
        devices = sizes[0] * sizes[1] * sizes[2]
        per = bands // GROUPS

        def call(*refs):
            refs = list(refs)
            head, rest = refs[:4], refs[4:]
            fields, rest = rest[:7], rest[7:]
            fys, rest = rest[:4], rest[4:]
            fyr, rest = rest[:4], rest[4:]
            fzs, rest = rest[:4], rest[4:]
            fzr, rest = rest[:4], rest[4:]
            kernel(sizes, *head, *fields, fys, fyr, fzs, fzr, *rest)

        depths = (2, 1, 2, 1)
        updated, trial = pl.pallas_call(
            call,
            out_shape=(
                jax.ShapeDtypeStruct(orbitals.shape, jnp.float32),
                jax.ShapeDtypeStruct(tile, jnp.float32),
            ),
            in_specs=[
                pl.BlockSpec(memory_space=pltpu.HBM),
                pl.BlockSpec(memory_space=pltpu.HBM),
            ],
            out_specs=(
                pl.BlockSpec(memory_space=pltpu.VMEM),
                pl.BlockSpec(memory_space=pltpu.VMEM),
            ),
            scratch_shapes=[field] * 5
            + [vmem(bands, xs, tiles), vmem(2 * COARSE_SWEEPS, GROUPS, xs // 2 + 4, tiles)]
            + [vmem(2, bands, d, tiles) for d in depths]
            + [vmem(2, bands, d, tiles) for d in depths]
            + [vmem(bands) for d in depths]
            + [vmem(2, bands) for d in depths]
            + [
                vmem(bands, xs, tiles),
                vmem(2 * COARSE_SWEEPS, GROUPS, xs // 2 + 2, tiles),
                vmem(4, GROUPS),
                vmem(4, 4, 2, GROUPS),
                vmem(4, GROUPS),
                vmem(QUAD, xs // 2 + 2, tiles),
                vmem(QUAD, xs // 2, tiles),
                vmem(QUAD, xs // 2),
                pltpu.VMEM((2, GROUPS, NDOTS * per, LANES), jnp.float32),
                pltpu.VMEM((5, bands, LANES), jnp.float32),
                vmem(3, GROUPS),
                pltpu.VMEM((2 * GROUPS, devices, 1, LANES), jnp.float32),
                pltpu.VMEM(potential.shape, jnp.float32),
                pltpu.VMEM(((8 * tiles + 2) * ROWS * per, LANES), jnp.float32),
                pltpu.SemaphoreType.DMA((GROUPS + 1, tiles)),
                pltpu.SemaphoreType.DMA((GROUPS,)),
                pltpu.SemaphoreType.DMA((2, GROUPS)),
                pltpu.SemaphoreType.DMA((2 * GROUPS,)),
                pltpu.SemaphoreType.DMA((2 * GROUPS,)),
                pltpu.SemaphoreType.REGULAR,
                pltpu.SemaphoreType.REGULAR,
            ],
            compiler_params=pltpu.CompilerParams(
                collective_id=0, has_side_effects=True, vmem_limit_bytes=53760 * 1024
            ),
        )(orbitals, potential)
        return updated, trial[:GROUPS, :per].reshape(bands)

    return jax.shard_map(
        body,
        mesh=mesh,
        in_specs=(P(None, "gx", "gy", "gz"), P("gx", "gy", "gz")),
        out_specs=(P(None, "gx", "gy", "gz"), P()),
        check_vma=False,
    )
```

```python
import functools
import math

import jax
import jax.numpy as jnp
from jax import lax
from jax.experimental import pallas as pl
from jax.experimental.pallas import tpu as pltpu
from jax.sharding import PartitionSpec as P

COARSE_SWEEPS = 4
QUAD = 4
AHEAD = 2
ENTRY = "b2"
ORDER = (
    "h0 b3 h1 h2",
    "r0 h3 r1 r2",
    "m0 r3 m1 m2",
    "f0 m3 f1 f2 f3",
    "H0 H1 H2 H3",
    "R0 R1 R2 R3",
    "M0 M1 M2 M3",
    "F0 F1 F2 F3",
)
WEIGHT = 0.8
COARSE_DIAG = 1.75
EPSILON = 1e-06
LANES = 128
ROWS = 8
GROUPS = 4
AXES = ("gx", "gy", "gz")
MESH = pl.DeviceIdType.MESH
NDOTS = 8


def kernel(sizes, orb_hbm, pot_hbm, out, energies, *scratch):
    (
        orb, app, res, cor, rsp, rem, coarse,
        fys, fyr, fzs, fzr, hy, beside, czs, czr, czm, dup, duph, dupz,
        acc, scal, keep, red, pot, blank, load_sem, send_sem, recv_sem, rsend, rrecv, greet_y, greet_z,
    ) = scratch
    nx, ny, nz = sizes
    bands, xs = orb_hbm.shape[0], orb_hbm.shape[1]
    tiles = orb_hbm.shape[3] // LANES
    xc = xs // 2
    per = bands // GROUPS
    devices = nx * ny * nz
    me = [lax.axis_index(a) for a in AXES]
    right = [lax.rem(m + 1, n) for m, n in zip(me, sizes)]
    left = [lax.rem(m + n - 1, n) for m, n in zip(me, sizes)]

    here = (me[0] * ny + me[1]) * nz + me[2]

    def start(copies):
        for c in copies:
            c.start()

    def wait(copies):
        for c in copies:
            c.wait()

    pot_load = pltpu.make_async_copy(pot_hbm, pot, load_sem.at[GROUPS, 0])

    def load_copies(g):
        part = pl.ds(g * per, per)
        return [
            pltpu.make_async_copy(
                orb_hbm.at[part, :, :, pl.ds(t * LANES, LANES)],
                orb.at[part, pl.ds(2, xs), t],
                load_sem.at[g, t],
            )
            for t in range(tiles)
        ]

    for g in range(GROUPS):
        start(load_copies(g))
    pot_load.start()

    def wrap(k, d):
        return lax.rem(me[k] + d, sizes[k])

    def every_peer(f):
        if devices <= 64:
            xyz = [[me[k]] + [wrap(k, d) for d in range(1, sizes[k])] for k in range(3)]
            for d in range(1, devices):
                f((xyz[0][d // (ny * nz)], xyz[1][d // nz % ny], xyz[2][d % nz]))
        else:

            def step(d, carry):
                f((wrap(0, d // (ny * nz)), wrap(1, lax.rem(d // nz, ny)), wrap(2, lax.rem(d, nz))))
                return carry

            lax.fori_loop(1, devices, step, 0)

    for level in (0, 2):
        for turn in range(2):
            for X in (0, 1 + xc):
                for g in range(GROUPS):
                    for t in range(tiles):
                        beside[turn * COARSE_SWEEPS + level, g, X, t] = jnp.zeros((ROWS, LANES), jnp.float32)

    def greet(semaphore, axes):
        for k in axes:
            for d in range(1, sizes[k]):
                pl.semaphore_signal(semaphore, inc=1, device_id={AXES[k]: wrap(k, d)}, device_id_type=MESH)

    def greeted(semaphore, axes):
        pl.semaphore_wait(semaphore, sum(sizes[k] - 1 for k in axes))

    barrier = pltpu.get_barrier_semaphore()
    greet(barrier, (0, 1, 2))

    row = lax.broadcasted_iota(jnp.int32, (ROWS, LANES), 0)
    lane = lax.broadcasted_iota(jnp.int32, (ROWS, LANES), 1)
    even_lane = lane % 2 == 0
    even_row = row % 2 == 0
    low_half = lane < LANES // 2
    first_of_four = lane % 4 < 2
    first_of_eight = lane % 8 < 4
    top_half = row < ROWS // 2

    z_ends = (right[2], left[2])[: 1 if nz == 2 else 2]

    def roll(v, k, axis):
        return pltpu.roll(v, k % v.shape[axis], axis)

    def flat(ref):
        n = 1
        for s in ref.shape[:-1]:
            n *= s
        return ref.reshape(n, LANES)

    def loop(lo, hi, f):
        def step(i, carry):
            f(i)
            return carry

        lax.fori_loop(lo, hi, step, 0)

    def send(moves, turn, g):
        for src, dst, to in moves:
            pltpu.make_async_remote_copy(
                src_ref=src,
                dst_ref=dst,
                send_sem=send_sem.at[g],
                recv_sem=recv_sem.at[turn % 2, g],
                device_id=to,
                device_id_type=MESH,
            ).start()

    def arrive(moves, turn, g):
        part = blank.at[pl.ds(0, sum(math.prod(src.shape) for src, _, _ in moves) // LANES)]
        pltpu.make_async_copy(part, part, recv_sem.at[turn % 2, g]).wait()
        pltpu.make_async_copy(part, part, send_sem.at[g]).wait()

    def fine_moves(field, which, depth, g):
        part = pl.ds(g * per, per)
        ys, yr = fys[which], fyr[which]
        zs, zr = fzs[which], fzr[which]
        moves = [
            (ys.at[0, part], yr.at[0, part], {"gy": right[1]}),
            (ys.at[1, part], yr.at[1, part], {"gy": left[1]}),
            (field.at[part, pl.ds(2 + xs - depth, depth)], field.at[part, pl.ds(2 - depth, depth)], {"gx": right[0]}),
            (field.at[part, pl.ds(2, depth)], field.at[part, pl.ds(2 + xs, depth)], {"gx": left[0]}),
        ]
        for end, z in enumerate(z_ends):
            moves.append((zs.at[part], zr.at[end, part], {"gz": z}))
        return moves

    def fine_pack(field, which, depth, g):
        view = flat(field)
        span = field.shape[1]
        ys, zs = fys[which], fzs[which]

        def pack(b):
            for t in range(tiles):
                for j in range(depth):
                    base = ((b * span + 2) * tiles + t) * ROWS
                    ys[0, b, j, t] = view[pl.ds(base + ROWS - depth + j, xs, stride=tiles * ROWS), :]
                    ys[1, b, j, t] = view[pl.ds(base + j, xs, stride=tiles * ROWS), :]
            packed = jnp.zeros((ROWS, LANES), jnp.float32)
            for x in range(xs):
                w = jnp.where(low_half, field[b, 2 + x, 0], field[b, 2 + x, tiles - 1])
                packed = jnp.where(lane // 4 == x, roll(w, 2 + 4 * x, 1), packed)
            zs[b] = packed

        for k in range(per):
            pack(g * per + k)

    def fine_send(field, which, depth, g):
        fine_pack(field, which, depth, g)
        send(fine_moves(field, which, depth, g), which, g)

    def fine_arrive(field, which, depth, g):
        arrive(fine_moves(field, which, depth, g), which, g)

    def z_packed(zr, b):
        if nz > 2:
            return jnp.where(first_of_four, zr[0, b], zr[1, b])
        return zr[0, b]

    def unpack_y(yr, b, depth):
        view = flat(hy)
        for t in range(tiles):
            for j in range(depth):
                base = (b * xs * tiles + t) * ROWS
                view[pl.ds(base + ROWS - depth + j, xs, stride=tiles * ROWS), :] = yr(0, j, t)
                view[pl.ds(base + j, xs, stride=tiles * ROWS), :] = yr(1, j, t)

    def shifted_y(v, h, k):
        up = roll(jnp.where(row >= ROWS - k, h, v), k, 0)
        down = roll(jnp.where(row < k, h, v), -k, 0)
        return up + down

    def shifted_z(vs, hz, k):
        before = [hz] + vs[:-1]
        after = vs[1:] + [hz]
        return [
            roll(jnp.where(lane >= LANES - k, p, v), k, 1) + roll(jnp.where(lane < k, n, v), -k, 1)
            for p, v, n in zip(before, vs, after)
        ]

    def hamiltonian(field, which, b, use):
        unpack_y(lambda s, j, t: fyr[which][s, b, j, t], b, 2)
        zp = z_packed(fzr[which], b)
        for x in range(xs):
            hz = roll(zp, -(4 * x + 2), 1)
            vs = [field[b, 2 + x, t] for t in range(tiles)]
            z1, z2 = shifted_z(vs, hz, 1), shifted_z(vs, hz, 2)
            outs = []
            for t in range(tiles):
                h = hy[b, x, t]
                near = field[b, 1 + x, t] + field[b, 3 + x, t] + shifted_y(vs[t], h, 1) + z1[t]
                far = field[b, x, t] + field[b, 4 + x, t] + shifted_y(vs[t], h, 2) + z2[t]
                potential = pot[x, :, t * LANES : (t + 1) * LANES]
                outs.append((potential + 3.75) * vs[t] - (2.0 / 3.0) * near + (1.0 / 24.0) * far)
            use(x, vs, outs)

    def rowsum(vs):
        return jnp.sum(functools.reduce(jnp.add, vs), axis=0, keepdims=True)

    def reduce_start(index, g, ndots):
        total = jnp.zeros((ROWS, LANES), jnp.float32)
        for i in range(ndots * per // ROWS):
            part = jnp.sum(acc[index, g, i * ROWS : (i + 1) * ROWS, :], axis=1, keepdims=True)
            total = jnp.where(lane == row + i * ROWS, part, total)
        k = index * GROUPS + g
        red[k, here] = jnp.sum(total, axis=0, keepdims=True)

        def send(to):
            pltpu.make_async_remote_copy(
                src_ref=red.at[k, here],
                dst_ref=red.at[k, here],
                send_sem=rsend.at[k],
                recv_sem=rrecv.at[k],
                device_id=to,
                device_id_type=MESH,
            ).start()

        every_peer(send)

    def reduce_finish(index, g, ndots):
        k = index * GROUPS + g
        rest = red.at[k, pl.ds(0, devices - 1)]
        pltpu.make_async_copy(rest, rest, rrecv.at[k]).wait()
        pltpu.make_async_copy(rest, rest, rsend.at[k]).wait()
        total = jnp.broadcast_to(jnp.sum(red[k], axis=0), (ROWS, LANES))
        return [total if q == 0 else roll(total, -q * per, 1) for q in range(ndots)]

    def put(k, g, values):
        for b in range(per):
            scal[k, pl.ds(g * per + b, 1), :] = jnp.broadcast_to(values[0:1, b : b + 1], (1, LANES))

    def get(k, b):
        return scal[k, pl.ds(b, 1), :]

    def restrict(b, ry, rz):
        k = lax.rem(b, QUAD)
        unpack_y(ry, b, 1)
        for X in range(xc):
            pair = [None] * tiles
            for x in (2 * X, 2 * X + 1):
                hz = roll(rz, -(4 * x + 2), 1)
                vs = [res[b, 2 + x, t] for t in range(tiles)]
                z1 = shifted_z(vs, hz, 1)
                for t in range(tiles):
                    s = res[b, 1 + x, t] + res[b, 3 + x, t] + shifted_y(vs[t], hy[b, x, t], 1) + z1[t]
                    m = (1.0 - WEIGHT) * vs[t] + (0.5 * WEIGHT / 4.0) * s
                    rem[b, x, t] = m
                    pair[t] = m if pair[t] is None else pair[t] + m
            for t in range(tiles):
                s = pair[t]
                s = s + jnp.where(even_row, roll(s, -1, 0), roll(s, 1, 0))
                s = s + jnp.where(even_lane, roll(s, -1, 1), roll(s, 1, 1))
                dup[k, 1 + X, t] = s * (0.125 * WEIGHT / COARSE_DIAG)

    def coarse_pack(level, g):
        for X in range(xc):
            for t in range(tiles):
                lanes = [jnp.where(even_lane, dup[k, 1 + X, t], dup[k + 1, 1 + X, t]) for k in (0, 2)]
                coarse[level, g, 2 + X, t] = jnp.where(even_row, lanes[0], lanes[1])

    def coarse_moves(level, w, g):
        own, side = coarse.at[level, g], beside.at[level, g]
        low, high = pl.ds(0, ROWS // 2), pl.ds(ROWS // 2, ROWS // 2)
        top, bottom = pl.ds(0, 2), pl.ds(ROWS - 2, 2)
        inner, last, first = pl.ds(2, xc), 1 + xc, 2
        right_x, left_x = {"gx": right[0]}, {"gx": left[0]}
        right_y, left_y = {"gy": right[1]}, {"gy": left[1]}
        moves = [
            (own.at[inner, :, high], side.at[pl.ds(1, xc), :, high], right_y),
            (own.at[inner, :, low], side.at[pl.ds(1, xc), :, low], left_y),
            (own.at[last, :, bottom], side.at[0, :, bottom], right_x | right_y),
            (own.at[last, :, top], side.at[0, :, top], right_x | left_y),
            (own.at[first, :, bottom], side.at[1 + xc, :, bottom], left_x | right_y),
            (own.at[first, :, top], side.at[1 + xc, :, top], left_x | left_y),
        ]
        for end, z in enumerate(z_ends):
            for part, to in ((bottom, right_y), (top, left_y)):
                moves.append((czs.at[w, g, part], czr.at[w, 3, end, g, part], to | {"gz": z}))
            for i, to in ((1, right_x), (2, left_x), (0, {})):
                moves.append((czs.at[w, g], czr.at[w, i, end, g], to | {"gz": z}))
        moves += [
            (own.at[pl.ds(xc, 2)], own.at[pl.ds(0, 2)], right_x),
            (own.at[pl.ds(2, 2)], own.at[pl.ds(2 + xc, 2)], left_x),
        ]
        return moves

    def coarse_send(level, w, g):
        packed = jnp.zeros((ROWS, LANES), jnp.float32)
        for X in range(xc):
            v = jnp.where(low_half, coarse[level, g, 2 + X, 0], coarse[level, g, 2 + X, tiles - 1])
            packed = jnp.where(lane // 8 == X, roll(v, 8 * X + 4, 1), packed)
        czs[w, g] = packed
        send(coarse_moves(level, w, g), w, g)

    def z_edges(w, i, g):
        if nz > 2:
            return jnp.where(first_of_eight, czr[w, i, 0, g], czr[w, i, 1, g])
        return czr[w, i, 0, g]

    def z_halo(packed, X):
        return roll(packed, -(8 * X + 4), 1)

    def update(v, s, rhs):
        return (1.0 - WEIGHT) * v + (0.125 * WEIGHT / COARSE_DIAG) * s + rhs

    def sweep_plane(zero, level, g, X, hz):
        vs = [coarse[level, g, 2 + X, t] for t in range(tiles)]
        z = shifted_z(vs, hz, 2)
        for t in range(tiles):
            s = coarse[level, g, 1 + X, t] + coarse[level, g, 3 + X, t]
            s = s + shifted_y(vs[t], beside[level, g, 1 + X, t], 2) + z[t]
            coarse[level + 1, g, 2 + X, t] = update(vs[t], s, coarse[zero, g, 2 + X, t])

    def sweep_wide(zero, level, w, g):
        zc, from_left, from_right, zy = (z_edges(w, i, g) for i in range(4))
        zs = czs[w, g]
        for X in range(-1, xc + 1):
            if X < 0:
                hz = z_halo(from_left, xc - 1)
            elif X == xc:
                hz = z_halo(from_right, 0)
            else:
                hz = z_halo(zc, X)
            sweep_plane(zero, level, g, X, hz)
        for X in range(xc):
            hs = [beside[level, g, 1 + X, t] for t in range(tiles)]
            z = shifted_z(hs, z_halo(zy, X), 2)
            for t in range(tiles):
                h, v = hs[t], coarse[level, g, 2 + X, t]
                y = jnp.where(top_half, roll(h, -2, 0) + roll(v, 2, 0), roll(h, 2, 0) + roll(v, -2, 0))
                s = beside[level, g, X, t] + beside[level, g, 2 + X, t] + y + z[t]
                beside[level + 1, g, 1 + X, t] = update(h, s, beside[zero, g, 1 + X, t])
        edge = 8 * (xc - 1)
        s = jnp.where(lane < 8, roll(from_left, -edge, 1), roll(zc, 8, 1))
        s = s + jnp.where(lane >= edge, roll(from_right, edge, 1), roll(zc, -8, 1))
        s = s + shifted_y(zc, zy, 2)
        s = s + jnp.where(
            first_of_eight, roll(zc, 2, 1) + roll(zs, -2, 1), roll(zc, -2, 1) + roll(zs, 2, 1)
        )
        czm[w, g] = update(zc, s, z_edges(w // 2 * 2, 0, g))

    def sweep_own(zero, level, w, g):
        zc = czm[w, g]
        for X in range(xc):
            sweep_plane(zero, level, g, X, z_halo(zc, X))

    def spread(p):
        out = []
        for v in (jnp.where(even_row, p, roll(p, 1, 0)), jnp.where(even_row, roll(p, -1, 0), p)):
            out.append(jnp.where(even_lane, v, roll(v, 1, 1)))
            out.append(jnp.where(even_lane, roll(v, -1, 1), v))
        return out

    def prolong(level, w, g, use):
        zc = czm[w, g]
        for X in range(xc + 2):
            for t in range(tiles):
                for k, v in enumerate(spread(coarse[level, g, 1 + X, t])):
                    dup[k, X, t] = v
        for X in range(xc):
            for t in range(tiles):
                for k, v in enumerate(spread(beside[level, g, 1 + X, t])):
                    duph[k, X, t] = v
            for k, v in enumerate(spread(z_halo(zc, X))):
                dupz[k, X] = v

        def one(b):
            k = lax.rem(b, QUAD)
            for X in range(xc):
                vs = [dup[k, 1 + X, t] for t in range(tiles)]
                z = shifted_z(vs, dupz[k, X], 1)
                for t in range(tiles):
                    s = shifted_y(vs[t], duph[k, X, t], 1) + z[t] + vs[t]
                    for x, other in ((2 * X, X), (2 * X + 1, 2 + X)):
                        total = s + dup[k, other, t]
                        kr = (1.0 - WEIGHT) * (res[b, 2 + x, t] + vs[t] + rem[b, x, t]) + (
                            0.5 * WEIGHT / 4.0
                        ) * total
                        use(b, x, t, kr)

        loop(g * per, (g + 1) * per, one)

    def apply_one(g, b):
        norm, energy = [], []

        def use(x, vs, outs):
            for t in range(tiles):
                app[b, 2 + x, t] = outs[t]
                norm.append(vs[t] * vs[t])
                energy.append(vs[t] * outs[t])

        hamiltonian(orb, 0, b, use)
        acc[0, g, pl.ds(b - g * per, 1), :] = rowsum(norm)
        acc[0, g, pl.ds(b - g * per + per, 1), :] = rowsum(energy)

    def prepare_first(b):
        e = get(0, b)
        for x in range(1, xs + 3):
            for t in range(tiles):
                res[b, x, t] = app[b, x, t] - e * orb[b, x, t]

        def ry(s, j, t):
            return fyr[1][s, b, 0, t] - e * fyr[0][s, b, 1 - s, t]

        restrict(b, ry, z_packed(fzr[1], b) - e * z_packed(fzr[0], b))

    def use_first(b, x, t, kr):
        cor[b, 2 + x, t] = kr

    def respond_one(g, b):
        e = get(0, b)
        dots = [None] * NDOTS

        def use(x, vs, outs):
            for t in range(tiles):
                c, o, r = vs[t], orb[b, 2 + x, t], res[b, 2 + x, t]
                p = outs[t] - e * c
                rsp[b, 2 + x, t] = p
                for q, (u, v) in enumerate(((r, p), (p, p), (o, c), (c, c), (p, o), (p, c), (r, o), (r, c))):
                    w = u * v
                    dots[q] = w if dots[q] is None else dots[q] + w

        hamiltonian(cor, 2, b, use)
        for q in range(NDOTS):
            acc[1, g, pl.ds(b - g * per + q * per, 1), :] = rowsum([dots[q]])

    def prepare_second(b):
        e, ml, mc, mcl = get(0, b), get(2, b), get(3, b), get(4, b)

        def mixed(r, p, o, c):
            return r + ml * p - mc * o - mcl * c

        for x in range(1, xs + 3):
            for t in range(tiles):
                res[b, x, t] = mixed(res[b, x, t], rsp[b, x, t], orb[b, x, t], cor[b, x, t])

        def ry(s, j, t):
            o = fyr[0][s, b, 1 - s, t]
            r = fyr[1][s, b, 0, t] - e * o
            return mixed(r, fyr[3][s, b, 0, t], o, fyr[2][s, b, 1 - s, t])

        oz = z_packed(fzr[0], b)
        rz = z_packed(fzr[1], b) - e * oz
        restrict(b, ry, mixed(rz, z_packed(fzr[3], b), oz, z_packed(fzr[2], b)))

    def use_second(b, x, t, kr):
        out[b, x, :, t * LANES : (t + 1) * LANES] = (
            orb[b, 2 + x, t] + get(2, b) * cor[b, 2 + x, t] + get(1, b) * kr
        )

    def coarse_begin(turn, g):
        coarse_pack(turn * COARSE_SWEEPS, g)
        coarse_send(turn * COARSE_SWEEPS, 2 * turn, g)

    def middle(turn, g):
        zero, w = turn * COARSE_SWEEPS, 2 * turn
        arrive(coarse_moves(zero, w, g), w, g)
        sweep_wide(zero, zero, w, g)
        sweep_own(zero, zero + 1, w, g)
        coarse_send(zero + 2, w + 1, g)

    def finish(turn, use, g):
        zero, w = turn * COARSE_SWEEPS, 2 * turn + 1
        arrive(coarse_moves(zero + 2, w, g), w, g)
        sweep_wide(zero, zero + 2, w, g)
        prolong(zero + 3, w, g, use)
        if turn == 0:
            fine_send(cor, 2, 2, g)

    def begin(g):
        wait(load_copies(g))
        fine_send(orb, 0, 2, g)

    def first_hamiltonian(g):
        fine_arrive(orb, 0, 2, g)
        loop(g * per, (g + 1) * per, functools.partial(apply_one, g))
        reduce_start(0, g, 2)
        fine_send(app, 1, 1, g)

    def first_residual(g):
        norm_orbitals, first_energy = reduce_finish(0, g, 2)
        energy = first_energy / (norm_orbitals + EPSILON)
        for i, v in enumerate((norm_orbitals, first_energy, energy)):
            keep[i, g] = v
        put(0, g, energy)
        fine_arrive(app, 1, 1, g)
        loop(g * per, (g + 1) * per, prepare_first)
        coarse_begin(0, g)

    def second_hamiltonian(g):
        fine_arrive(cor, 2, 2, g)
        loop(g * per, (g + 1) * per, functools.partial(respond_one, g))
        reduce_start(1, g, NDOTS)
        fine_send(rsp, 3, 1, g)

    def second_residual(g):
        norm_orbitals, first_energy, energy = (keep[i, g] for i in range(3))
        rp, pp, oc, cc, po, pc, ro, rc = reduce_finish(1, g, NDOTS)
        lam = -rp / (pp + EPSILON)
        trial_norm = norm_orbitals + 2.0 * lam * oc + lam * lam * cc
        trial_sum = (
            first_energy + lam * ((po + energy * oc) + (rc + energy * oc)) + lam * lam * (pc + energy * cc)
        )
        trial = trial_sum / (trial_norm + EPSILON)
        energies[pl.ds(g, 1), :] = trial[0:1]
        change = trial - energy
        projected = lam * rp - change * (ro + lam * rc)
        cross = po + lam * pc
        change_norm = lam * lam * pp - 2.0 * lam * change * cross + change * change * trial_norm
        mix = -projected / (change_norm + EPSILON)
        put(1, g, lam)
        put(2, g, mix * lam)
        put(3, g, mix * change)
        put(4, g, mix * change * lam)
        fine_arrive(rsp, 3, 1, g)
        loop(g * per, (g + 1) * per, prepare_second)
        coarse_begin(1, g)

    for g in range(AHEAD):
        wait(load_copies(g))
        fine_pack(orb, 0, 2, g)
    greeted(barrier, (0, 1, 2))
    for g in range(AHEAD):
        send(fine_moves(orb, 0, 2, g), 0, g)
    greet(greet_y, (1,))
    stages = dict(
        b=begin,
        h=first_hamiltonian,
        r=first_residual,
        m=functools.partial(middle, 0),
        f=functools.partial(finish, 0, use_first),
        H=second_hamiltonian,
        R=second_residual,
        M=functools.partial(middle, 1),
        F=functools.partial(finish, 1, use_second),
    )

    def run(steps):
        steps = steps.split()
        while steps:
            name, lo = steps[0][0], int(steps[0][1])
            n = 1
            while n < len(steps) and steps[n] == f"{name}{lo + n}":
                n += 1
            loop(lo, lo + n, stages[name])
            steps = steps[n:]

    run(ENTRY)
    greeted(greet_y, (1,))
    greet(greet_z, (2,))
    pot_load.wait()
    greeted(greet_z, (2,))
    for steps in ORDER:
        run(steps)


def solution(mesh):
    sizes = tuple(mesh.shape[a] for a in AXES)

    def body(orbitals, potential):
        bands, xs, ys, zs = orbitals.shape
        tiles = zs // LANES
        tile = (ROWS, LANES)
        vmem = lambda *s: pltpu.VMEM(s + tile, jnp.float32)
        field = vmem(bands, xs + 4, tiles)
        assert bands == QUAD * GROUPS
        devices = sizes[0] * sizes[1] * sizes[2]
        per = bands // GROUPS

        def call(*refs):
            refs = list(refs)
            head, rest = refs[:4], refs[4:]
            fields, rest = rest[:7], rest[7:]
            fys, rest = rest[:4], rest[4:]
            fyr, rest = rest[:4], rest[4:]
            fzs, rest = rest[:4], rest[4:]
            fzr, rest = rest[:4], rest[4:]
            kernel(sizes, *head, *fields, fys, fyr, fzs, fzr, *rest)

        depths = (2, 1, 2, 1)
        updated, trial = pl.pallas_call(
            call,
            out_shape=(
                jax.ShapeDtypeStruct(orbitals.shape, jnp.float32),
                jax.ShapeDtypeStruct(tile, jnp.float32),
            ),
            in_specs=[
                pl.BlockSpec(memory_space=pltpu.HBM),
                pl.BlockSpec(memory_space=pltpu.HBM),
            ],
            out_specs=(
                pl.BlockSpec(memory_space=pltpu.VMEM),
                pl.BlockSpec(memory_space=pltpu.VMEM),
            ),
            scratch_shapes=[field] * 5
            + [vmem(bands, xs, tiles), vmem(2 * COARSE_SWEEPS, GROUPS, xs // 2 + 4, tiles)]
            + [vmem(2, bands, d, tiles) for d in depths]
            + [vmem(2, bands, d, tiles) for d in depths]
            + [vmem(bands) for d in depths]
            + [vmem(2, bands) for d in depths]
            + [
                vmem(bands, xs, tiles),
                vmem(2 * COARSE_SWEEPS, GROUPS, xs // 2 + 2, tiles),
                vmem(4, GROUPS),
                vmem(4, 4, 2, GROUPS),
                vmem(4, GROUPS),
                vmem(QUAD, xs // 2 + 2, tiles),
                vmem(QUAD, xs // 2, tiles),
                vmem(QUAD, xs // 2),
                pltpu.VMEM((2, GROUPS, NDOTS * per, LANES), jnp.float32),
                pltpu.VMEM((5, bands, LANES), jnp.float32),
                vmem(3, GROUPS),
                pltpu.VMEM((2 * GROUPS, devices, 1, LANES), jnp.float32),
                pltpu.VMEM(potential.shape, jnp.float32),
                pltpu.VMEM(((8 * tiles + 2) * ROWS * per, LANES), jnp.float32),
                pltpu.SemaphoreType.DMA((GROUPS + 1, tiles)),
                pltpu.SemaphoreType.DMA((GROUPS,)),
                pltpu.SemaphoreType.DMA((2, GROUPS)),
                pltpu.SemaphoreType.DMA((2 * GROUPS,)),
                pltpu.SemaphoreType.DMA((2 * GROUPS,)),
                pltpu.SemaphoreType.REGULAR,
                pltpu.SemaphoreType.REGULAR,
            ],
            compiler_params=pltpu.CompilerParams(
                collective_id=0, has_side_effects=True, vmem_limit_bytes=53760 * 1024
            ),
        )(orbitals, potential)
        return updated, trial[:GROUPS, :per].reshape(bands)

    return jax.shard_map(
        body,
        mesh=mesh,
        in_specs=(P(None, "gx", "gy", "gz"), P("gx", "gy", "gz")),
        out_specs=(P(None, "gx", "gy", "gz"), P()),
        check_vma=False,
    )
```

```python
import functools
import math

import jax
import jax.numpy as jnp
from jax import lax
from jax.experimental import pallas as pl
from jax.experimental.pallas import tpu as pltpu
from jax.sharding import PartitionSpec as P

COARSE_SWEEPS = 4
QUAD = 4
AHEAD = 2
ENTRY = "b2"
ORDER = (
    "h0 b3 h1 h2",
    "r0 h3 r1 r2",
    "m0 r3 m1 m2",
    "f0 m3 f1 f2 f3",
    "H0 H1 H2 H3",
    "R0 R1 R2 R3",
    "M0 M1 M2 M3",
    "F0 F1 F2 F3",
)
WEIGHT = 0.8
COARSE_DIAG = 1.75
EPSILON = 1e-06
LANES = 128
ROWS = 8
GROUPS = 4
AXES = ("gx", "gy", "gz")
MESH = pl.DeviceIdType.MESH
NDOTS = 8


def kernel(sizes, orb_hbm, pot_hbm, out, energies, *scratch):
    (
        orb, app, res, cor, rsp, rem, coarse,
        fys, fyr, fzs, fzr, hy, beside, czs, czr, czm, dup, duph, dupz,
        acc, scal, keep, red, pot, blank, load_sem, send_sem, recv_sem, rsend, rrecv, greet_y, greet_z,
    ) = scratch
    nx, ny, nz = sizes
    bands, xs = orb_hbm.shape[0], orb_hbm.shape[1]
    tiles = orb_hbm.shape[3] // LANES
    xc = xs // 2
    per = bands // GROUPS
    devices = nx * ny * nz
    me = [lax.axis_index(a) for a in AXES]
    right = [lax.rem(m + 1, n) for m, n in zip(me, sizes)]
    left = [lax.rem(m + n - 1, n) for m, n in zip(me, sizes)]

    here = (me[0] * ny + me[1]) * nz + me[2]

    def start(copies):
        for c in copies:
            c.start()

    def wait(copies):
        for c in copies:
            c.wait()

    pot_load = pltpu.make_async_copy(pot_hbm, pot, load_sem.at[GROUPS, 0])

    def load_copies(g):
        part = pl.ds(g * per, per)
        return [
            pltpu.make_async_copy(
                orb_hbm.at[part, :, :, pl.ds(t * LANES, LANES)],
                orb.at[part, pl.ds(2, xs), t],
                load_sem.at[g, t],
            )
            for t in range(tiles)
        ]

    for g in range(GROUPS):
        start(load_copies(g))
    pot_load.start()

    def wrap(k, d):
        return lax.rem(me[k] + d, sizes[k])

    def every_peer(f):
        if devices <= 64:
            xyz = [[me[k]] + [wrap(k, d) for d in range(1, sizes[k])] for k in range(3)]
            for d in range(1, devices):
                f((xyz[0][d // (ny * nz)], xyz[1][d // nz % ny], xyz[2][d % nz]))
        else:

            def step(d, carry):
                f((wrap(0, d // (ny * nz)), wrap(1, lax.rem(d // nz, ny)), wrap(2, lax.rem(d, nz))))
                return carry

            lax.fori_loop(1, devices, step, 0)

    for level in (0, 2):
        for turn in range(2):
            for X in (0, 1 + xc):
                for g in range(GROUPS):
                    for t in range(tiles):
                        beside[turn * COARSE_SWEEPS + level, g, X, t] = jnp.zeros((ROWS, LANES), jnp.float32)

    def greet(semaphore, axes):
        for k in axes:
            for d in range(1, sizes[k]):
                pl.semaphore_signal(semaphore, inc=1, device_id={AXES[k]: wrap(k, d)}, device_id_type=MESH)

    def greeted(semaphore, axes):
        pl.semaphore_wait(semaphore, sum(sizes[k] - 1 for k in axes))

    barrier = pltpu.get_barrier_semaphore()
    greet(barrier, (0, 1, 2))

    row = lax.broadcasted_iota(jnp.int32, (ROWS, LANES), 0)
    lane = lax.broadcasted_iota(jnp.int32, (ROWS, LANES), 1)
    even_lane = lane % 2 == 0
    even_row = row % 2 == 0
    low_half = lane < LANES // 2
    first_of_four = lane % 4 < 2
    first_of_eight = lane % 8 < 4
    top_half = row < ROWS // 2

    z_ends = (right[2], left[2])[: 1 if nz == 2 else 2]

    def roll(v, k, axis):
        return pltpu.roll(v, k % v.shape[axis], axis)

    def flat(ref):
        n = 1
        for s in ref.shape[:-1]:
            n *= s
        return ref.reshape(n, LANES)

    def loop(lo, hi, f):
        def step(i, carry):
            f(i)
            return carry

        lax.fori_loop(lo, hi, step, 0)

    def send(moves, turn, g):
        for src, dst, to in moves:
            pltpu.make_async_remote_copy(
                src_ref=src,
                dst_ref=dst,
                send_sem=send_sem.at[g],
                recv_sem=recv_sem.at[turn % 2, g],
                device_id=to,
                device_id_type=MESH,
            ).start()

    def arrive(moves, turn, g):
        part = blank.at[pl.ds(0, sum(math.prod(src.shape) for src, _, _ in moves) // LANES)]
        pltpu.make_async_copy(part, part, recv_sem.at[turn % 2, g]).wait()
        pltpu.make_async_copy(part, part, send_sem.at[g]).wait()

    def fine_moves(field, which, depth, g):
        part = pl.ds(g * per, per)
        ys, yr = fys[which], fyr[which]
        zs, zr = fzs[which], fzr[which]
        moves = [
            (ys.at[0, part], yr.at[0, part], {"gy": right[1]}),
            (ys.at[1, part], yr.at[1, part], {"gy": left[1]}),
            (field.at[part, pl.ds(2 + xs - depth, depth)], field.at[part, pl.ds(2 - depth, depth)], {"gx": right[0]}),
            (field.at[part, pl.ds(2, depth)], field.at[part, pl.ds(2 + xs, depth)], {"gx": left[0]}),
        ]
        for end, z in enumerate(z_ends):
            moves.append((zs.at[part], zr.at[end, part], {"gz": z}))
        return moves

    def fine_pack(field, which, depth, g):
        view = flat(field)
        span = field.shape[1]
        ys, zs = fys[which], fzs[which]

        def pack(b):
            for t in range(tiles):
                for j in range(depth):
                    base = ((b * span + 2) * tiles + t) * ROWS
                    ys[0, b, j, t] = view[pl.ds(base + ROWS - depth + j, xs, stride=tiles * ROWS), :]
                    ys[1, b, j, t] = view[pl.ds(base + j, xs, stride=tiles * ROWS), :]
            packed = jnp.zeros((ROWS, LANES), jnp.float32)
            for x in range(xs):
                w = jnp.where(low_half, field[b, 2 + x, 0], field[b, 2 + x, tiles - 1])
                packed = jnp.where(lane // 4 == x, roll(w, 2 + 4 * x, 1), packed)
            zs[b] = packed

        for k in range(per):
            pack(g * per + k)

    def fine_send(field, which, depth, g):
        fine_pack(field, which, depth, g)
        send(fine_moves(field, which, depth, g), which, g)

    def fine_arrive(field, which, depth, g):
        arrive(fine_moves(field, which, depth, g), which, g)

    def z_packed(zr, b):
        if nz > 2:
            return jnp.where(first_of_four, zr[0, b], zr[1, b])
        return zr[0, b]

    def unpack_y(yr, b, depth):
        view = flat(hy)
        for t in range(tiles):
            for j in range(depth):
                base = (b * xs * tiles + t) * ROWS
                view[pl.ds(base + ROWS - depth + j, xs, stride=tiles * ROWS), :] = yr(0, j, t)
                view[pl.ds(base + j, xs, stride=tiles * ROWS), :] = yr(1, j, t)

    def shifted_y(v, h, k):
        up = roll(jnp.where(row >= ROWS - k, h, v), k, 0)
        down = roll(jnp.where(row < k, h, v), -k, 0)
        return up + down

    def shifted_z(vs, hz, k):
        before = [hz] + vs[:-1]
        after = vs[1:] + [hz]
        return [
            roll(jnp.where(lane >= LANES - k, p, v), k, 1) + roll(jnp.where(lane < k, n, v), -k, 1)
            for p, v, n in zip(before, vs, after)
        ]

    def hamiltonian(field, which, b, use):
        unpack_y(lambda s, j, t: fyr[which][s, b, j, t], b, 2)
        zp = z_packed(fzr[which], b)
        for x in range(xs):
            hz = roll(zp, -(4 * x + 2), 1)
            vs = [field[b, 2 + x, t] for t in range(tiles)]
            z1, z2 = shifted_z(vs, hz, 1), shifted_z(vs, hz, 2)
            outs = []
            for t in range(tiles):
                h = hy[b, x, t]
                near = field[b, 1 + x, t] + field[b, 3 + x, t] + shifted_y(vs[t], h, 1) + z1[t]
                far = field[b, x, t] + field[b, 4 + x, t] + shifted_y(vs[t], h, 2) + z2[t]
                potential = pot[x, :, t * LANES : (t + 1) * LANES]
                outs.append((potential + 3.75) * vs[t] - (2.0 / 3.0) * near + (1.0 / 24.0) * far)
            use(x, vs, outs)

    def rowsum(vs):
        return jnp.sum(functools.reduce(jnp.add, vs), axis=0, keepdims=True)

    def reduce_start(index, g, ndots):
        total = jnp.zeros((ROWS, LANES), jnp.float32)
        for i in range(ndots * per // ROWS):
            part = jnp.sum(acc[index, g, i * ROWS : (i + 1) * ROWS, :], axis=1, keepdims=True)
            total = jnp.where(lane == row + i * ROWS, part, total)
        k = index * GROUPS + g
        red[k, here] = jnp.sum(total, axis=0, keepdims=True)

        def send(to):
            pltpu.make_async_remote_copy(
                src_ref=red.at[k, here],
                dst_ref=red.at[k, here],
                send_sem=rsend.at[k],
                recv_sem=rrecv.at[k],
                device_id=to,
                device_id_type=MESH,
            ).start()

        every_peer(send)

    def reduce_finish(index, g, ndots):
        k = index * GROUPS + g
        rest = red.at[k, pl.ds(0, devices - 1)]
        pltpu.make_async_copy(rest, rest, rrecv.at[k]).wait()
        pltpu.make_async_copy(rest, rest, rsend.at[k]).wait()
        total = jnp.broadcast_to(jnp.sum(red[k], axis=0), (ROWS, LANES))
        return [total if q == 0 else roll(total, -q * per, 1) for q in range(ndots)]

    def put(k, g, values):
        for b in range(per):
            scal[k, pl.ds(g * per + b, 1), :] = jnp.broadcast_to(values[0:1, b : b + 1], (1, LANES))

    def get(k, b):
        return scal[k, pl.ds(b, 1), :]

    def restrict(b, ry, rz):
        k = lax.rem(b, QUAD)
        unpack_y(ry, b, 1)
        for X in range(xc):
            pair = [None] * tiles
            for x in (2 * X, 2 * X + 1):
                hz = roll(rz, -(4 * x + 2), 1)
                vs = [res[b, 2 + x, t] for t in range(tiles)]
                z1 = shifted_z(vs, hz, 1)
                for t in range(tiles):
                    s = res[b, 1 + x, t] + res[b, 3 + x, t] + shifted_y(vs[t], hy[b, x, t], 1) + z1[t]
                    m = (1.0 - WEIGHT) * vs[t] + (0.5 * WEIGHT / 4.0) * s
                    rem[b, x, t] = m
                    pair[t] = m if pair[t] is None else pair[t] + m
            for t in range(tiles):
                s = pair[t]
                s = s + jnp.where(even_row, roll(s, -1, 0), roll(s, 1, 0))
                s = s + jnp.where(even_lane, roll(s, -1, 1), roll(s, 1, 1))
                dup[k, 1 + X, t] = s * (0.125 * WEIGHT / COARSE_DIAG)

    def coarse_pack(level, g):
        for X in range(xc):
            for t in range(tiles):
                lanes = [jnp.where(even_lane, dup[k, 1 + X, t], dup[k + 1, 1 + X, t]) for k in (0, 2)]
                coarse[level, g, 2 + X, t] = jnp.where(even_row, lanes[0], lanes[1])

    def coarse_moves(level, w, g):
        own, side = coarse.at[level, g], beside.at[level, g]
        low, high = pl.ds(0, ROWS // 2), pl.ds(ROWS // 2, ROWS // 2)
        top, bottom = pl.ds(0, 2), pl.ds(ROWS - 2, 2)
        inner, last, first = pl.ds(2, xc), 1 + xc, 2
        right_x, left_x = {"gx": right[0]}, {"gx": left[0]}
        right_y, left_y = {"gy": right[1]}, {"gy": left[1]}
        moves = [
            (own.at[inner, :, high], side.at[pl.ds(1, xc), :, high], right_y),
            (own.at[inner, :, low], side.at[pl.ds(1, xc), :, low], left_y),
            (own.at[last, :, bottom], side.at[0, :, bottom], right_x | right_y),
            (own.at[last, :, top], side.at[0, :, top], right_x | left_y),
            (own.at[first, :, bottom], side.at[1 + xc, :, bottom], left_x | right_y),
            (own.at[first, :, top], side.at[1 + xc, :, top], left_x | left_y),
        ]
        for end, z in enumerate(z_ends):
            for part, to in ((bottom, right_y), (top, left_y)):
                moves.append((czs.at[w, g, part], czr.at[w, 3, end, g, part], to | {"gz": z}))
            for i, to in ((1, right_x), (2, left_x), (0, {})):
                moves.append((czs.at[w, g], czr.at[w, i, end, g], to | {"gz": z}))
        moves += [
            (own.at[pl.ds(xc, 2)], own.at[pl.ds(0, 2)], right_x),
            (own.at[pl.ds(2, 2)], own.at[pl.ds(2 + xc, 2)], left_x),
        ]
        return moves

    def coarse_send(level, w, g):
        packed = jnp.zeros((ROWS, LANES), jnp.float32)
        for X in range(xc):
            v = jnp.where(low_half, coarse[level, g, 2 + X, 0], coarse[level, g, 2 + X, tiles - 1])
            packed = jnp.where(lane // 8 == X, roll(v, 8 * X + 4, 1), packed)
        czs[w, g] = packed
        send(coarse_moves(level, w, g), w, g)

    def z_edges(w, i, g):
        if nz > 2:
            return jnp.where(first_of_eight, czr[w, i, 0, g], czr[w, i, 1, g])
        return czr[w, i, 0, g]

    def z_halo(packed, X):
        return roll(packed, -(8 * X + 4), 1)

    def update(v, s, rhs):
        return (1.0 - WEIGHT) * v + (0.125 * WEIGHT / COARSE_DIAG) * s + rhs

    def sweep_plane(zero, level, g, X, hz):
        vs = [coarse[level, g, 2 + X, t] for t in range(tiles)]
        z = shifted_z(vs, hz, 2)
        for t in range(tiles):
            s = coarse[level, g, 1 + X, t] + coarse[level, g, 3 + X, t]
            s = s + shifted_y(vs[t], beside[level, g, 1 + X, t], 2) + z[t]
            coarse[level + 1, g, 2 + X, t] = update(vs[t], s, coarse[zero, g, 2 + X, t])

    def sweep_wide(zero, level, w, g):
        zc, from_left, from_right, zy = (z_edges(w, i, g) for i in range(4))
        zs = czs[w, g]
        for X in range(-1, xc + 1):
            if X < 0:
                hz = z_halo(from_left, xc - 1)
            elif X == xc:
                hz = z_halo(from_right, 0)
            else:
                hz = z_halo(zc, X)
            sweep_plane(zero, level, g, X, hz)
        for X in range(xc):
            hs = [beside[level, g, 1 + X, t] for t in range(tiles)]
            z = shifted_z(hs, z_halo(zy, X), 2)
            for t in range(tiles):
                h, v = hs[t], coarse[level, g, 2 + X, t]
                y = jnp.where(top_half, roll(h, -2, 0) + roll(v, 2, 0), roll(h, 2, 0) + roll(v, -2, 0))
                s = beside[level, g, X, t] + beside[level, g, 2 + X, t] + y + z[t]
                beside[level + 1, g, 1 + X, t] = update(h, s, beside[zero, g, 1 + X, t])
        edge = 8 * (xc - 1)
        s = jnp.where(lane < 8, roll(from_left, -edge, 1), roll(zc, 8, 1))
        s = s + jnp.where(lane >= edge, roll(from_right, edge, 1), roll(zc, -8, 1))
        s = s + shifted_y(zc, zy, 2)
        s = s + jnp.where(
            first_of_eight, roll(zc, 2, 1) + roll(zs, -2, 1), roll(zc, -2, 1) + roll(zs, 2, 1)
        )
        czm[w, g] = update(zc, s, z_edges(w // 2 * 2, 0, g))

    def sweep_own(zero, level, w, g):
        zc = czm[w, g]
        for X in range(xc):
            sweep_plane(zero, level, g, X, z_halo(zc, X))

    def spread(p):
        out = []
        for v in (jnp.where(even_row, p, roll(p, 1, 0)), jnp.where(even_row, roll(p, -1, 0), p)):
            out.append(jnp.where(even_lane, v, roll(v, 1, 1)))
            out.append(jnp.where(even_lane, roll(v, -1, 1), v))
        return out

    def prolong(level, w, g, use):
        zc = czm[w, g]
        for X in range(xc + 2):
            for t in range(tiles):
                for k, v in enumerate(spread(coarse[level, g, 1 + X, t])):
                    dup[k, X, t] = v
        for X in range(xc):
            for t in range(tiles):
                for k, v in enumerate(spread(beside[level, g, 1 + X, t])):
                    duph[k, X, t] = v
            for k, v in enumerate(spread(z_halo(zc, X))):
                dupz[k, X] = v

        def one(b):
            k = lax.rem(b, QUAD)
            for X in range(xc):
                vs = [dup[k, 1 + X, t] for t in range(tiles)]
                z = shifted_z(vs, dupz[k, X], 1)
                for t in range(tiles):
                    s = shifted_y(vs[t], duph[k, X, t], 1) + z[t] + vs[t]
                    for x, other in ((2 * X, X), (2 * X + 1, 2 + X)):
                        total = s + dup[k, other, t]
                        kr = (1.0 - WEIGHT) * (res[b, 2 + x, t] + vs[t] + rem[b, x, t]) + (
                            0.5 * WEIGHT / 4.0
                        ) * total
                        use(b, x, t, kr)

        loop(g * per, (g + 1) * per, one)

    def apply_one(g, b):
        norm, energy = [], []

        def use(x, vs, outs):
            for t in range(tiles):
                app[b, 2 + x, t] = outs[t]
                norm.append(vs[t] * vs[t])
                energy.append(vs[t] * outs[t])

        hamiltonian(orb, 0, b, use)
        acc[0, g, pl.ds(b - g * per, 1), :] = rowsum(norm)
        acc[0, g, pl.ds(b - g * per + per, 1), :] = rowsum(energy)

    def prepare_first(b):
        e = get(0, b)
        for x in range(1, xs + 3):
            for t in range(tiles):
                res[b, x, t] = app[b, x, t] - e * orb[b, x, t]

        def ry(s, j, t):
            return fyr[1][s, b, 0, t] - e * fyr[0][s, b, 1 - s, t]

        restrict(b, ry, z_packed(fzr[1], b) - e * z_packed(fzr[0], b))

    def use_first(b, x, t, kr):
        cor[b, 2 + x, t] = kr

    def respond_one(g, b):
        e = get(0, b)
        dots = [None] * NDOTS

        def use(x, vs, outs):
            for t in range(tiles):
                c, o, r = vs[t], orb[b, 2 + x, t], res[b, 2 + x, t]
                p = outs[t] - e * c
                rsp[b, 2 + x, t] = p
                for q, (u, v) in enumerate(((r, p), (p, p), (o, c), (c, c), (p, o), (p, c), (r, o), (r, c))):
                    w = u * v
                    dots[q] = w if dots[q] is None else dots[q] + w

        hamiltonian(cor, 2, b, use)
        for q in range(NDOTS):
            acc[1, g, pl.ds(b - g * per + q * per, 1), :] = rowsum([dots[q]])

    def prepare_second(b):
        e, ml, mc, mcl = get(0, b), get(2, b), get(3, b), get(4, b)

        def mixed(r, p, o, c):
            return r + ml * p - mc * o - mcl * c

        for x in range(1, xs + 3):
            for t in range(tiles):
                res[b, x, t] = mixed(res[b, x, t], rsp[b, x, t], orb[b, x, t], cor[b, x, t])

        def ry(s, j, t):
            o = fyr[0][s, b, 1 - s, t]
            r = fyr[1][s, b, 0, t] - e * o
            return mixed(r, fyr[3][s, b, 0, t], o, fyr[2][s, b, 1 - s, t])

        oz = z_packed(fzr[0], b)
        rz = z_packed(fzr[1], b) - e * oz
        restrict(b, ry, mixed(rz, z_packed(fzr[3], b), oz, z_packed(fzr[2], b)))

    def use_second(b, x, t, kr):
        out[b, x, :, t * LANES : (t + 1) * LANES] = (
            orb[b, 2 + x, t] + get(2, b) * cor[b, 2 + x, t] + get(1, b) * kr
        )

    def coarse_begin(turn, g):
        coarse_pack(turn * COARSE_SWEEPS, g)
        coarse_send(turn * COARSE_SWEEPS, 2 * turn, g)

    def middle(turn, g):
        zero, w = turn * COARSE_SWEEPS, 2 * turn
        arrive(coarse_moves(zero, w, g), w, g)
        sweep_wide(zero, zero, w, g)
        sweep_own(zero, zero + 1, w, g)
        coarse_send(zero + 2, w + 1, g)

    def finish(turn, use, g):
        zero, w = turn * COARSE_SWEEPS, 2 * turn + 1
        arrive(coarse_moves(zero + 2, w, g), w, g)
        sweep_wide(zero, zero + 2, w, g)
        prolong(zero + 3, w, g, use)
        if turn == 0:
            fine_send(cor, 2, 2, g)

    def begin(g):
        wait(load_copies(g))
        fine_send(orb, 0, 2, g)

    def first_hamiltonian(g):
        fine_arrive(orb, 0, 2, g)
        loop(g * per, (g + 1) * per, functools.partial(apply_one, g))
        reduce_start(0, g, 2)
        fine_send(app, 1, 1, g)

    def first_residual(g):
        norm_orbitals, first_energy = reduce_finish(0, g, 2)
        energy = first_energy / (norm_orbitals + EPSILON)
        for i, v in enumerate((norm_orbitals, first_energy, energy)):
            keep[i, g] = v
        put(0, g, energy)
        fine_arrive(app, 1, 1, g)
        loop(g * per, (g + 1) * per, prepare_first)
        coarse_begin(0, g)

    def second_hamiltonian(g):
        fine_arrive(cor, 2, 2, g)
        loop(g * per, (g + 1) * per, functools.partial(respond_one, g))
        reduce_start(1, g, NDOTS)
        fine_send(rsp, 3, 1, g)

    def second_residual(g):
        norm_orbitals, first_energy, energy = (keep[i, g] for i in range(3))
        rp, pp, oc, cc, po, pc, ro, rc = reduce_finish(1, g, NDOTS)
        lam = -rp / (pp + EPSILON)
        trial_norm = norm_orbitals + 2.0 * lam * oc + lam * lam * cc
        trial_sum = (
            first_energy + lam * ((po + energy * oc) + (rc + energy * oc)) + lam * lam * (pc + energy * cc)
        )
        trial = trial_sum / (trial_norm + EPSILON)
        keep[3, g] = trial
        change = trial - energy
        projected = lam * rp - change * (ro + lam * rc)
        cross = po + lam * pc
        change_norm = lam * lam * pp - 2.0 * lam * change * cross + change * change * trial_norm
        mix = -projected / (change_norm + EPSILON)
        put(1, g, lam)
        put(2, g, mix * lam)
        put(3, g, mix * change)
        put(4, g, mix * change * lam)
        fine_arrive(rsp, 3, 1, g)
        loop(g * per, (g + 1) * per, prepare_second)
        coarse_begin(1, g)

    for g in range(AHEAD):
        wait(load_copies(g))
        fine_pack(orb, 0, 2, g)
    greeted(barrier, (0, 1, 2))
    for g in range(AHEAD):
        send(fine_moves(orb, 0, 2, g), 0, g)
    greet(greet_y, (1,))
    stages = dict(
        b=begin,
        h=first_hamiltonian,
        r=first_residual,
        m=functools.partial(middle, 0),
        f=functools.partial(finish, 0, use_first),
        H=second_hamiltonian,
        R=second_residual,
        M=functools.partial(middle, 1),
        F=functools.partial(finish, 1, use_second),
    )

    def run(steps):
        steps = steps.split()
        while steps:
            name, lo = steps[0][0], int(steps[0][1])
            n = 1
            while n < len(steps) and steps[n] == f"{name}{lo + n}":
                n += 1
            loop(lo, lo + n, stages[name])
            steps = steps[n:]

    run(ENTRY)
    greeted(greet_y, (1,))
    greet(greet_z, (2,))
    pot_load.wait()
    greeted(greet_z, (2,))
    for steps in ORDER:
        run(steps)
    trial = keep[3, 0]
    for g in range(1, GROUPS):
        trial = jnp.where(lane // per == g, roll(keep[3, g], g * per, 1), trial)
    energies[...] = trial[0, :bands]


def solution(mesh):
    sizes = tuple(mesh.shape[a] for a in AXES)

    def body(orbitals, potential):
        bands, xs, ys, zs = orbitals.shape
        tiles = zs // LANES
        tile = (ROWS, LANES)
        vmem = lambda *s: pltpu.VMEM(s + tile, jnp.float32)
        field = vmem(bands, xs + 4, tiles)
        assert bands == QUAD * GROUPS
        devices = sizes[0] * sizes[1] * sizes[2]
        per = bands // GROUPS

        def call(*refs):
            refs = list(refs)
            head, rest = refs[:4], refs[4:]
            fields, rest = rest[:7], rest[7:]
            fys, rest = rest[:4], rest[4:]
            fyr, rest = rest[:4], rest[4:]
            fzs, rest = rest[:4], rest[4:]
            fzr, rest = rest[:4], rest[4:]
            kernel(sizes, *head, *fields, fys, fyr, fzs, fzr, *rest)

        depths = (2, 1, 2, 1)
        updated, trial = pl.pallas_call(
            call,
            out_shape=(
                jax.ShapeDtypeStruct(orbitals.shape, jnp.float32),
                jax.ShapeDtypeStruct((bands,), jnp.float32),
            ),
            in_specs=[
                pl.BlockSpec(memory_space=pltpu.HBM),
                pl.BlockSpec(memory_space=pltpu.HBM),
            ],
            out_specs=(
                pl.BlockSpec(memory_space=pltpu.VMEM),
                pl.BlockSpec(memory_space=pltpu.VMEM),
            ),
            scratch_shapes=[field] * 5
            + [vmem(bands, xs, tiles), vmem(2 * COARSE_SWEEPS, GROUPS, xs // 2 + 4, tiles)]
            + [vmem(2, bands, d, tiles) for d in depths]
            + [vmem(2, bands, d, tiles) for d in depths]
            + [vmem(bands) for d in depths]
            + [vmem(2, bands) for d in depths]
            + [
                vmem(bands, xs, tiles),
                vmem(2 * COARSE_SWEEPS, GROUPS, xs // 2 + 2, tiles),
                vmem(4, GROUPS),
                vmem(4, 4, 2, GROUPS),
                vmem(4, GROUPS),
                vmem(QUAD, xs // 2 + 2, tiles),
                vmem(QUAD, xs // 2, tiles),
                vmem(QUAD, xs // 2),
                pltpu.VMEM((2, GROUPS, NDOTS * per, LANES), jnp.float32),
                pltpu.VMEM((5, bands, LANES), jnp.float32),
                vmem(4, GROUPS),
                pltpu.VMEM((2 * GROUPS, devices, 1, LANES), jnp.float32),
                pltpu.VMEM(potential.shape, jnp.float32),
                pltpu.VMEM(((8 * tiles + 2) * ROWS * per, LANES), jnp.float32),
                pltpu.SemaphoreType.DMA((GROUPS + 1, tiles)),
                pltpu.SemaphoreType.DMA((GROUPS,)),
                pltpu.SemaphoreType.DMA((2, GROUPS)),
                pltpu.SemaphoreType.DMA((2 * GROUPS,)),
                pltpu.SemaphoreType.DMA((2 * GROUPS,)),
                pltpu.SemaphoreType.REGULAR,
                pltpu.SemaphoreType.REGULAR,
            ],
            compiler_params=pltpu.CompilerParams(
                collective_id=0, has_side_effects=True, vmem_limit_bytes=53760 * 1024
            ),
        )(orbitals, potential)
        return updated, trial

    return jax.shard_map(
        body,
        mesh=mesh,
        in_specs=(P(None, "gx", "gy", "gz"), P("gx", "gy", "gz")),
        out_specs=(P(None, "gx", "gy", "gz"), P()),
        check_vma=False,
    )
```
